128 devices in a mesh: section: 8 (over y, core), sim: 16 (over z, x).
Axes of the slice: x: 4, y: 4, z: 4, core: 2. Of those that a mesh axis runs over, the one named last changes fastest.
Arguments:
- state: float32 [256, 64, 16384], P('section', None, 'sim'), may hold values from -60 to 60
- owner: int32 [256, 1], P('section'), may hold values from 0 to 15; in each aligned block of 32 rows (0 to 31, 32 to 63, ...) at most 4 rows name the same one
- counts: int32 [256], P('section'), may hold values from 4096 to 16384
Outputs:
- slab_mean: float32 [256, 64], P('section')
- slab_cov: float32 [256, 4096], P('section', 'sim')
- group_cov: float32 [128, 4096], P(('section', 'sim'))
- global_mean: float32 [64], replicated
- global_cov: float32 [64, 64], replicated
The draws below stay inside these ranges and needn't reach their ends.
Inputs may be any that keep to these rules, and one draw needn't show every extreme that they name: Among the 32 slabs of one group, no owner is named by more than 4 slabs, and one owner is named by exactly 4 slabs in some or all groups.
All inputs are finite; a program needn't handle non-finite values.
Results may differ from the reference program's by a relative error of at most 0.0003.
Values sent between devices are 32-bit elements; how exact they have to be, the bound alone decides.
A program may use at most 64 MiB of HBM per device.

```python
import math
import jax
import jax.numpy as jnp
import numpy as np
from jax import lax

V = 64
SL = 32
CAP = 4
NSLAB = 256
CELLS = 16384
GROUPS = 128
N_SIM = 16


def draw_state(key, part):
    keys = jax.random.split(jax.random.fold_in(key, 11), 5)
    shape = (NSLAB, V, CELLS)
    base = jnp.clip(jax.random.normal(keys[0], shape, jnp.float32), -4.0, 4.0)
    slab_scale = (1.0 + 2.0 * jnp.arange(NSLAB, dtype=jnp.float32) / max(NSLAB - 1, 1)).reshape(NSLAB, 1, 1)
    mixing = jnp.eye(V, dtype=jnp.float32) + 0.5 * jax.random.normal(keys[2], (V, V), jnp.float32) / math.sqrt(V)
    var_scale = jnp.exp(jax.random.uniform(keys[3], (V,), jnp.float32, math.log(0.5), math.log(2.0)))
    offset = jax.random.uniform(keys[4], (NSLAB, V, 1), jnp.float32, -2.0, 2.0)
    cell_scale = 1.0 + 2.0 * jnp.arange(CELLS, dtype=jnp.float32) / CELLS
    mixed = jnp.einsum('vw,swc->svc', mixing, base)
    values = mixed * var_scale[None, :, None] * slab_scale * cell_scale[None, None, :] + offset
    return jnp.clip(values, -60.0, 60.0)


def place_ends(values, key, smallest, largest):
    extent = values.shape
    spot = [jax.random.randint(jax.random.fold_in(key, axis), (), 0, extent[axis]) for axis in range(len(extent))]
    values = values.at[tuple(spot)].set(smallest)
    longest = extent.index(max(extent))
    spot[longest] = (spot[longest] + 1) % extent[longest]
    return values.at[tuple(spot)].set(largest)


def assign_block(stream_key, own, number, rows, amount, top, most, skew):
    order = jax.random.permutation(stream_key, amount)
    heavy_load, usual = portions_of(amount, rows * top, most, skew, True), portions_of(amount, rows * top, most, skew, False)
    places = jnp.arange(amount)

    def named(lengths, offset_by):
        used = int((lengths > 0).sum())
        fixed = max(1, used // 4)
        shifted = fixed + (places - fixed + offset_by * (used - fixed)) % max(1, amount - fixed)
        return jnp.zeros((amount,), jnp.int32).at[order[jnp.where(places < fixed, places, shifted)]].set(jnp.asarray(lengths, jnp.int32))

    lengths = jnp.where(number % 4 == 0, named(heavy_load, number // 4), named(usual, number - number // 4 - 1))
    mixed = jax.random.permutation(jax.random.fold_in(own, 3), amount)
    source_of, receiver = mixed[0:amount // 2 * 2:2], mixed[1:amount // 2 * 2:2]
    room = jnp.minimum(lengths[source_of] - 1, most - lengths[receiver]) // 2
    room = jnp.where((source_of == order[0]) | (receiver == order[0]) | (lengths[receiver] == 0), 0, jnp.maximum(room, 0))
    shifted = jax.random.randint(jax.random.fold_in(own, 4), (amount // 2,), 0, 1 << 20) % (room + 1)
    lengths = lengths.at[source_of].add(-shifted).at[receiver].add(shifted)
    items = jnp.searchsorted(jnp.cumsum(lengths), jnp.arange(rows * top), side="right").astype(jnp.int32)
    table = items.reshape(top, rows).T
    table = table[jax.random.permutation(jax.random.fold_in(own, 1), rows)]
    offset_by = jax.random.randint(jax.random.fold_in(own, 2), (rows, 1), 0, top)
    return jnp.take_along_axis(table, (jnp.arange(top)[None, :] + offset_by) % top, axis=1)


def portions_of(number_of, total, reach, skew, full):
    loads = [(1 << 20) // math.isqrt(standing ** skew) + 1 for standing in range(1, number_of + 1)]
    largest = reach if full else min(reach, max(-(-total // number_of), total * loads[0] // sum(loads)))
    least = 1 if total - largest >= number_of - 1 else 0
    given, surplus = [largest] + [least] * (number_of - 1), total - largest - least * (number_of - 1)
    while surplus > 0:
        candidates = [i for i in range(1, number_of) if given[i] < largest] or [i for i in range(1, number_of) if given[i] < reach]
        pool, budget = sum([loads[i] for i in candidates]), surplus
        for i in candidates:
            extra = min(reach - given[i], max(1, budget * loads[i] // pool), surplus)
            given[i] = given[i] + extra
            surplus = surplus - extra
    return np.array(given)


def setup_inputs(seed: int = 0) -> dict:
    arg_keys = jax.random.split(jax.random.key(seed), 4)
    state = draw_state(jax.random.fold_in(arg_keys[3], 71), 0)
    owner_keys = jax.random.split(jax.random.fold_in(arg_keys[1], 1), NSLAB // SL)
    owner_turns = jax.random.permutation(jax.random.fold_in(arg_keys[1], 3), NSLAB // SL)
    owner = jax.vmap(lambda own, number: assign_block(jax.random.fold_in(arg_keys[1], 2), own, number, SL, N_SIM, 1, CAP, 2))(owner_keys, owner_turns).reshape((NSLAB, 1))
    counts = place_ends(jax.random.randint(arg_keys[2], (NSLAB,), CELLS // 4, CELLS + 1), jax.random.fold_in(arg_keys[2], 1), CELLS // 4, CELLS).astype(jnp.int32)
    return {"state": state, "owner": owner, "counts": counts}


def one_slab(pair):
    block, count = pair
    live = jnp.arange(CELLS, dtype=jnp.int32) < count
    number = count.astype(jnp.float32)
    mean = jnp.sum(jnp.where(live[None, :], block, 0.0), axis=1) / number
    centered = jnp.where(live[None, :], block - mean[:, None], 0.0)
    comoment = jnp.dot(centered, centered.T, precision=lax.Precision.HIGHEST, preferred_element_type=jnp.float32)
    return mean, comoment


def reference(state, owner, counts):
    slab_mean, comoment = lax.map(one_slab, (state, counts))
    number = counts.astype(jnp.float32)
    slab_cov = (comoment / (number - 1.0)[:, None, None]).reshape(NSLAB, V * V)
    slab_index = jnp.arange(NSLAB, dtype=jnp.int32)
    group = (slab_index // SL) * N_SIM + owner[:, 0].astype(jnp.int32)
    member = (group[:, None] == jnp.arange(GROUPS, dtype=jnp.int32)[None, :]).astype(jnp.float32)
    high = lax.Precision.HIGHEST
    group_count = jnp.dot(number, member, precision=high)
    group_mean = jnp.dot(member.T, number[:, None] * slab_mean, precision=high) / jnp.maximum(group_count, 1.0)[:, None]
    offset = slab_mean - jnp.dot(member, group_mean, precision=high)
    inner = comoment + number[:, None, None] * offset[:, :, None] * offset[:, None, :]
    group_comoment = jnp.dot(member.T, inner.reshape(NSLAB, V * V), precision=high)
    group_cov = group_comoment / jnp.maximum(group_count - 1.0, 1.0)[:, None]
    total = jnp.sum(number)
    global_mean = jnp.sum(number[:, None] * slab_mean, axis=0) / total
    gap = slab_mean - global_mean[None, :]
    spread = jnp.sum(comoment + number[:, None, None] * gap[:, :, None] * gap[:, None, :], axis=0)
    global_cov = spread / (total - 1.0)
    return slab_mean, slab_cov, group_cov, global_mean, global_cov
```

```python
import functools

import jax
import jax.numpy as jnp
from jax import lax
from jax.experimental import pallas as pl
from jax.experimental.pallas import tpu as pltpu
from jax.sharding import PartitionSpec as P

MESH = pl.DeviceIdType.MESH
HIGH = lax.Precision.HIGHEST
F32 = jnp.float32
BF16 = jnp.bfloat16


def dot_rows(a, b):
    return lax.dot_general(a, b, (((1,), (1,)), ((), ())), preferred_element_type=F32)


def dot_high(a, b):
    return jnp.dot(a, b, precision=HIGH, preferred_element_type=F32)


def iota(shape, dim):
    return lax.broadcasted_iota(jnp.int32, shape, dim)


def kernel(
    n_sec, n_sim, width, chunks,
    state, counts, owner,
    mean_out, cov_out, grp_out, gmean_out, gcov_out,
    xv, meanb, cobuf, sums, sq, sendb, recvb, qbuf, qrecv, zrecv, frecv, gsend, grecv, grp, corrb, n64, own64, turn, turn2,
    load_sem, send_sem, sums_sem, piece_sem, q_sem, z_sem, f_sem, g_sem,
):
    pairs, _, cells = xv.shape
    half = pairs // 2
    sec = lax.axis_index("section")
    me = lax.axis_index("sim")
    z, x = me // 4, me % 4
    base = me * cells

    def sim_peer(k):
        return ((z + k // 4) % 4) * 4 + (x + k % 4) % 4

    def sec_peer(k):
        return (sec + k) % n_sec

    loads = [pltpu.make_async_copy(state.at[p], xv.at[p], load_sem.at[p]) for p in range(pairs)]
    for c in loads:
        c.start()

    barrier = pltpu.get_barrier_semaphore()
    for k in range(1, n_sim):
        pl.semaphore_signal(barrier, inc=1, device_id=(sec, sim_peer(k)), device_id_type=MESH)
    for k in range(1, n_sec):
        pl.semaphore_signal(barrier, inc=1, device_id=(sec_peer(k), me), device_id_type=MESH)

    lane8, sub8 = iota((8, 128), 1), iota((8, 128), 0)
    left8, first8 = lane8 < width, sub8 % 2 == 0
    for i in range(half):
        def spread(ref):
            return jnp.where(
                left8,
                jnp.where(first8, ref[4 * i], ref[4 * i + 2]),
                jnp.where(first8, ref[4 * i + 1], ref[4 * i + 3]),
            )
        n64[8 * i:8 * i + 8, :] = spread(counts).astype(F32)
        own64[8 * i:8 * i + 8, :] = spread(owner)
    lane16, sub16 = iota((pairs, 128), 1), iota((pairs, 128), 0)
    left16 = lane16 < width
    c_even = jnp.zeros((pairs, 128), jnp.int32)
    c_odd, o_even, o_odd = c_even, c_even, c_even
    for p in range(pairs):
        here = sub16 == p
        c_even = jnp.where(here, counts[2 * p], c_even)
        c_odd = jnp.where(here, counts[2 * p + 1], c_odd)
        o_even = jnp.where(here, owner[2 * p], o_even)
        o_odd = jnp.where(here, owner[2 * p + 1], o_odd)
    n_int = jnp.where(left16, c_even, c_odd)
    n_all = n_int.astype(F32)
    n_loc = jnp.clip(n_int - base, 0, cells).astype(F32)

    lane_c = iota((1, cells), 1)
    lane128 = iota((128, 128), 1)

    def first(p, cols):
        pltpu.make_async_copy(state.at[p], xv.at[p], load_sem.at[p]).wait()
        got = []
        for h in range(2):
            n = jnp.clip(counts[2 * p + h] - base, 0, cells)
            block = xv[p, h * width:(h + 1) * width, :]
            s = jnp.sum(jnp.where(lane_c < n, block, 0.0), axis=1, keepdims=True)
            s = jnp.broadcast_to(s, (width, 128))
            meanb[p, h * width:(h + 1) * width, :] = s / jnp.maximum(n, 1).astype(F32)
            got.append(s)
        return jnp.where(lane128 == p, jnp.concatenate(got, axis=0), cols)

    cols = lax.fori_loop(0, pairs, first, jnp.zeros((128, 128), F32))
    mine = cols.T[0:pairs, :]
    sums[me] = mine

    pl.semaphore_wait(barrier, n_sim - 1 + n_sec - 1)
    for k in range(1, n_sim):
        pltpu.make_async_remote_copy(
            sums.at[me], sums.at[me], send_sem.at[0], sums_sem,
            device_id=(sec, sim_peer(k)), device_id_type=MESH,
        ).start()

    left64 = iota((width, 128), 1) < width

    def second(p, carry):
        hi, lo = [], []
        for h in range(2):
            n = jnp.clip(counts[2 * p + h] - base, 0, cells)
            rows = pl.ds(h * width, width)
            m = meanb[p, rows, :]
            m = jnp.concatenate([m] * (cells // 128), axis=1)
            c = jnp.where(lane_c < n, xv[p, rows, :] - m, 0.0)
            top = c.astype(BF16)
            hi.append(top)
            lo.append((c - top.astype(F32)).astype(BF16))
        hi = jnp.concatenate(hi, axis=0)
        lo = jnp.concatenate(lo, axis=0)
        both = dot_rows(hi, jnp.concatenate([hi, lo], axis=0))
        cross = both[:, 128:256]
        full = both[:, 0:128] + cross + cross.T
        cobuf[p] = jnp.where(left64, full[0:width, :], full[width:, :])
        return carry

    lax.fori_loop(0, pairs, second, 0)

    pltpu.make_async_copy(sums.at[pl.ds(0, n_sim - 1)], sums.at[pl.ds(0, n_sim - 1)], sums_sem).wait()
    total = sums[0]
    for d in range(1, n_sim):
        total = total + sums[d]
    means = total / n_all
    shift = mine / jnp.maximum(n_loc, 1.0) - means
    sq[...] = jnp.zeros((128, 128), F32)
    sq[0:pairs, :] = shift
    col_shift = sq[...].T
    row_shift = shift * n_loc

    qsum = jnp.zeros((width, 128), F32)
    per = half // chunks
    for p in range(pairs):
        i, pp = p // 2, p % 2
        c = jnp.where(left64, col_shift[0:width, p:p + 1], col_shift[width:, p:p + 1])
        co = cobuf[p] + c * row_shift[p:p + 1, :]
        qsum = qsum + co
        sendb[i, pl.ds(pp, width, stride=2), :] = co
        if pp == 1 and (i + 1) % per == 0:
            t = i // per
            for k in range(1, n_sim):
                to = sim_peer(k)
                pltpu.make_async_remote_copy(
                    sendb.at[pl.ds(t * per, per), pl.ds(pl.multiple_of(8 * to, 8), 8), :],
                    recvb.at[me, pl.ds(t * per, per)],
                    send_sem.at[1], piece_sem.at[t],
                    device_id=(sec, to), device_id_type=MESH,
                ).start()
    recvb[me] = sendb[:, pl.ds(pl.multiple_of(8 * me, 8), 8), :]

    swapped = pltpu.roll(means, width, 1)
    m_even = jnp.where(left16, means, swapped)
    m_odd = jnp.where(left16, swapped, means)
    cf_even, cf_odd = c_even.astype(F32), c_odd.astype(F32)

    def about(w_even, w_odd, least):
        count = jnp.sum(w_even, axis=0, keepdims=True) + jnp.sum(w_odd, axis=0, keepdims=True)
        weighted = jnp.sum(w_even * m_even, axis=0, keepdims=True) + jnp.sum(w_odd * m_odd, axis=0, keepdims=True)
        mean = weighted / jnp.maximum(count, least)
        d_even, d_odd = m_even - mean, m_odd - mean
        off = jnp.concatenate([d_even, d_odd], axis=0)
        left = jnp.concatenate([w_even * d_even, w_odd * d_odd], axis=0)
        return count, weighted, dot_high(left.T, off)[0:width, :]

    sec_count, sec_sum, sec_co = about(cf_even, cf_odd, 1.0)
    q = qsum + pltpu.roll(qsum, width, 1) + sec_co * (1.0 / n_sim)
    rows8 = jnp.where(sub8 == 0, sec_sum, jnp.where(sub8 == 1, sec_count, 0.0))
    for s in range(n_sec):
        qbuf[s, 0:8, :] = q[8 * s:8 * s + 8, :]
        qbuf[s, 8:16, :] = rows8
    for k in range(1, n_sec):
        to = sec_peer(k)
        pltpu.make_async_remote_copy(
            qbuf.at[to], qrecv.at[sec], send_sem.at[2], q_sem,
            device_id=(to, me), device_id_type=MESH,
        ).start()
    qrecv[sec] = qbuf[sec]

    turn[pl.ds(0, pairs, stride=2), :] = means
    turn[pl.ds(1, pairs, stride=2), :] = swapped
    mean_out[...] = turn[:, 0:width]
    grp_count, _, grp_co = about(
        jnp.where(o_even == me, cf_even, 0.0), jnp.where(o_odd == me, cf_odd, 0.0), 1.0
    )
    corrb[...] = grp_co
    left32 = iota((width // 2, 128), 1) < width
    between = jnp.where(left32, corrb[pl.ds(0, width // 2, stride=2), :], corrb[pl.ds(1, width // 2, stride=2), :])
    lane64, sub64 = iota((width, 128), 1), iota((width, 128), 0)
    names = jnp.where(
        ((sub64 % 8) // 2 == (lane64 % width) // n_sim) & (own64[...] == lane64 % n_sim), 1.0, 0.0
    ).T
    gsend[...] = jnp.zeros((8 * n_sim, 128), F32)

    pltpu.make_async_copy(qrecv.at[pl.ds(0, n_sec - 1)], qrecv.at[pl.ds(0, n_sec - 1)], q_sem).wait()
    part = qrecv[0, 0:8, :]
    sec_sums, sec_counts = qrecv[0, 8:9, :], qrecv[0, 9:10, :]
    sums_l, counts_l = [sec_sums], [sec_counts]
    for s in range(1, n_sec):
        part = part + qrecv[s, 0:8, :]
        sums_l.append(qrecv[s, 8:9, :])
        counts_l.append(qrecv[s, 9:10, :])
    sec_sums, sec_counts = jnp.concatenate(sums_l, axis=0), jnp.concatenate(counts_l, axis=0)
    zrecv[me] = part
    for k in range(1, n_sim):
        pltpu.make_async_remote_copy(
            zrecv.at[me], zrecv.at[me], send_sem.at[3], z_sem,
            device_id=(sec, sim_peer(k)), device_id_type=MESH,
        ).start()
    all_count = jnp.sum(sec_counts, axis=0, keepdims=True)
    all_mean = jnp.sum(sec_sums, axis=0, keepdims=True) / all_count
    gap = sec_sums / sec_counts - all_mean
    spread_co = dot_high((sec_counts * gap).T, gap)[0:width, :]
    gmean_out[...] = all_mean

    for t in range(chunks):
        pltpu.make_async_copy(
            recvb.at[pl.ds(0, n_sim - 1), pl.ds(0, per)], recvb.at[pl.ds(0, n_sim - 1), pl.ds(0, per)],
            piece_sem.at[t],
        ).wait()
    co = recvb[0]
    for d in range(1, n_sim):
        co = co + recvb[d]
    co = co.reshape(width, 128)
    named = dot_high(names, co)
    g = jnp.where(left64, named[0:width, :], named[width:, :])
    g = g + pltpu.roll(g, width, 1)
    gsend[pl.ds(0, n_sim, stride=8), :] = jnp.where(left16, g[0:16, :], g[16:32, :])
    gsend[pl.ds(1, n_sim, stride=8), :] = jnp.where(left16, g[32:48, :], g[48:64, :])
    mine8 = pl.ds(pl.multiple_of(8 * me, 8), 8)
    for k in range(1, n_sim):
        to = sim_peer(k)
        pltpu.make_async_remote_copy(
            gsend.at[pl.ds(pl.multiple_of(8 * to, 8), 8), :], grecv.at[mine8, :], send_sem.at[4], g_sem,
            device_id=(sec, to), device_id_type=MESH,
        ).start()
    grecv[mine8, :] = gsend[mine8, :]

    corrb[...] = co / (n64[...] - 1.0)
    for pp in range(2):
        for rr in range(2):
            a = corrb[pl.ds(4 * rr + pp, 8, stride=8), :]
            b = corrb[pl.ds(4 * rr + 2 + pp, 8, stride=8), :]
            turned = turn if rr == 0 else turn2
            turned[pl.ds(2 * pp, 8, stride=4), :] = jnp.where(left8, a, pltpu.roll(b, width, 1))
            turned[pl.ds(2 * pp + 1, 8, stride=4), :] = jnp.where(left8, pltpu.roll(a, width, 1), b)
    cov_out[:, 0:128] = turn[...]
    cov_out[:, 128:256] = turn2[...]

    pltpu.make_async_copy(zrecv.at[pl.ds(0, n_sim - 1)], zrecv.at[pl.ds(0, n_sim - 1)], z_sem).wait()
    part = zrecv[0]
    for d in range(1, n_sim):
        part = part + zrecv[d]
    frecv[sec] = part
    for k in range(1, n_sec):
        pltpu.make_async_remote_copy(
            frecv.at[sec], frecv.at[sec], send_sem.at[5], f_sem,
            device_id=(sec_peer(k), me), device_id_type=MESH,
        ).start()

    pltpu.make_async_copy(
        grecv.at[pl.ds(0, 8 * (n_sim - 1)), :], grecv.at[pl.ds(0, 8 * (n_sim - 1)), :], g_sem
    ).wait()
    grp[pl.ds(0, n_sim, stride=2), :] = grecv[pl.ds(0, n_sim, stride=8), :]
    grp[pl.ds(1, n_sim, stride=2), :] = grecv[pl.ds(1, n_sim, stride=8), :]
    grp_out[...] = (grp[...] + between) / jnp.maximum(grp_count - 1.0, 1.0)

    pltpu.make_async_copy(frecv.at[pl.ds(0, n_sec - 1)], frecv.at[pl.ds(0, n_sec - 1)], f_sem).wait()
    whole = frecv[...].reshape(width, 128)
    gcov_out[...] = ((whole + spread_co) / (all_count - 1.0))[:, 0:width]

    def sent(ref, n, sem):
        pltpu.make_async_copy(ref.at[pl.ds(0, n)], ref.at[pl.ds(0, n)], sem).wait()

    sent(sums, n_sim - 1, send_sem.at[0])
    sent(recvb, n_sim - 1, send_sem.at[1])
    sent(qrecv, n_sec - 1, send_sem.at[2])
    sent(zrecv, n_sim - 1, send_sem.at[3])
    sent(grecv, 8 * (n_sim - 1), send_sem.at[4])
    sent(frecv, n_sec - 1, send_sem.at[5])


def solution(mesh):
    n_sec, n_sim = mesh.shape["section"], mesh.shape["sim"]
    chunks = 2

    def local(state, owner, counts):
        slabs, width, cells = state.shape
        pairs = slabs // 2
        half = pairs // 2
        vmem = pl.BlockSpec(memory_space=pltpu.VMEM)
        smem = pl.BlockSpec(memory_space=pltpu.SMEM)
        dma = pltpu.SemaphoreType.DMA
        mean, cov, grp, gmean, gcov = pl.pallas_call(
            functools.partial(kernel, n_sec, n_sim, width, chunks),
            out_shape=[
                jax.ShapeDtypeStruct((slabs, width), F32),
                jax.ShapeDtypeStruct((slabs, width * width // n_sim), F32),
                jax.ShapeDtypeStruct((width // 2, 2 * width), F32),
                jax.ShapeDtypeStruct((1, 2 * width), F32),
                jax.ShapeDtypeStruct((width, width), F32),
            ],
            in_specs=[pl.BlockSpec(memory_space=pl.ANY), smem, smem],
            out_specs=[vmem] * 5,
            scratch_shapes=[
                pltpu.VMEM((pairs, 2 * width, cells), F32),
                pltpu.VMEM((pairs, 2 * width, 128), F32),
                pltpu.VMEM((pairs, width, 128), F32),
                pltpu.VMEM((n_sim, pairs, 128), F32),
                pltpu.VMEM((128, 128), F32),
                pltpu.VMEM((half, 2 * width, 128), F32),
                pltpu.VMEM((n_sim, half, 8, 128), F32),
                pltpu.VMEM((n_sec, 16, 128), F32),
                pltpu.VMEM((n_sec, 16, 128), F32),
                pltpu.VMEM((n_sim, 8, 128), F32),
                pltpu.VMEM((n_sec, 8, 128), F32),
                pltpu.VMEM((8 * n_sim, 128), F32),
                pltpu.VMEM((8 * n_sim, 128), F32),
                pltpu.VMEM((width // 2, 128), F32),
                pltpu.VMEM((width, 128), F32),
                pltpu.VMEM((width, 128), F32),
                pltpu.VMEM((width, 128), jnp.int32),
                pltpu.VMEM((slabs, 128), F32),
                pltpu.VMEM((slabs, 128), F32),
                dma((pairs,)),
                dma((6,)),
                dma(()),
                dma((chunks,)),
                dma(()),
                dma(()),
                dma(()),
                dma(()),
            ],
            compiler_params=pltpu.CompilerParams(
                collective_id=0, has_side_effects=True, vmem_limit_bytes=32 * 1024 * 1024
            ),
            name="moments",
        )(state.reshape(pairs, 2 * width, cells), counts, owner.reshape(slabs))
        return mean, cov, grp.reshape(1, width * width), gmean[0, :width], gcov

    return jax.shard_map(
        local,
        mesh=mesh,
        in_specs=(P("section", None, "sim"), P("section", None), P("section")),
        out_specs=(P("section", None), P("section", "sim"), P(("section", "sim"), None), P(), P()),
        check_vma=False,
    )
```

```python
import functools

import jax
import jax.numpy as jnp
from jax import lax
from jax.experimental import pallas as pl
from jax.experimental.pallas import tpu as pltpu
from jax.sharding import PartitionSpec as P

MESH = pl.DeviceIdType.MESH
HIGH = lax.Precision.HIGHEST
F32 = jnp.float32
BF16 = jnp.bfloat16


def dot_rows(a, b):
    return lax.dot_general(a, b, (((1,), (1,)), ((), ())), preferred_element_type=F32)


def dot_high(a, b):
    return jnp.dot(a, b, precision=HIGH, preferred_element_type=F32)


def iota(shape, dim):
    return lax.broadcasted_iota(jnp.int32, shape, dim)


def kernel(
    n_sec, n_sim, width, chunks,
    state, counts_hbm, owner_hbm,
    mean_out, cov_out, grp_out, gmean_out, gcov_out,
    xv, meanb, cobuf, sums, sq, sendb, recvb, qbuf, qrecv, zrecv, frecv, gsend, grecv, grp, corrb, n64, own64, turn, turn2,
    counts, owner, load_sem, int_sem, send_sem, sums_sem, piece_sem, q_sem, z_sem, f_sem, g_sem,
):
    pairs, _, cells = xv.shape
    half = pairs // 2
    sec = lax.axis_index("section")
    me = lax.axis_index("sim")
    z, x = me // 4, me % 4
    base = me * cells

    def sim_peer(k):
        return ((z + k // 4) % 4) * 4 + (x + k % 4) % 4

    def sec_peer(k):
        return (sec + k) % n_sec

    loads = [pltpu.make_async_copy(state.at[p], xv.at[p], load_sem.at[p]) for p in range(pairs)]
    small = [
        pltpu.make_async_copy(counts_hbm, counts, int_sem.at[0]),
        pltpu.make_async_copy(owner_hbm, owner, int_sem.at[1]),
    ]
    for c in small + loads:
        c.start()

    barrier = pltpu.get_barrier_semaphore()
    for k in range(1, n_sim):
        pl.semaphore_signal(barrier, inc=1, device_id=(sec, sim_peer(k)), device_id_type=MESH)
    for k in range(1, n_sec):
        pl.semaphore_signal(barrier, inc=1, device_id=(sec_peer(k), me), device_id_type=MESH)

    for c in small:
        c.wait()

    lane8, sub8 = iota((8, 128), 1), iota((8, 128), 0)
    left8, first8 = lane8 < width, sub8 % 2 == 0
    for i in range(half):
        def spread(ref):
            return jnp.where(
                left8,
                jnp.where(first8, ref[4 * i], ref[4 * i + 2]),
                jnp.where(first8, ref[4 * i + 1], ref[4 * i + 3]),
            )
        n64[8 * i:8 * i + 8, :] = spread(counts).astype(F32)
        own64[8 * i:8 * i + 8, :] = spread(owner)
    lane16, sub16 = iota((pairs, 128), 1), iota((pairs, 128), 0)
    left16 = lane16 < width
    c_even = jnp.zeros((pairs, 128), jnp.int32)
    c_odd, o_even, o_odd = c_even, c_even, c_even
    for p in range(pairs):
        here = sub16 == p
        c_even = jnp.where(here, counts[2 * p], c_even)
        c_odd = jnp.where(here, counts[2 * p + 1], c_odd)
        o_even = jnp.where(here, owner[2 * p], o_even)
        o_odd = jnp.where(here, owner[2 * p + 1], o_odd)
    n_int = jnp.where(left16, c_even, c_odd)
    n_all = n_int.astype(F32)
    n_loc = jnp.clip(n_int - base, 0, cells).astype(F32)

    lane_c = iota((1, cells), 1)
    lane128 = iota((128, 128), 1)

    def first(p, cols):
        pltpu.make_async_copy(state.at[p], xv.at[p], load_sem.at[p]).wait()
        got = []
        for h in range(2):
            n = jnp.clip(counts[2 * p + h] - base, 0, cells)
            block = xv[p, h * width:(h + 1) * width, :]
            s = jnp.sum(jnp.where(lane_c < n, block, 0.0), axis=1, keepdims=True)
            s = jnp.broadcast_to(s, (width, 128))
            meanb[p, h * width:(h + 1) * width, :] = s / jnp.maximum(n, 1).astype(F32)
            got.append(s)
        return jnp.where(lane128 == p, jnp.concatenate(got, axis=0), cols)

    cols = lax.fori_loop(0, pairs, first, jnp.zeros((128, 128), F32))
    mine = cols.T[0:pairs, :]
    sums[me] = mine

    pl.semaphore_wait(barrier, n_sim - 1 + n_sec - 1)
    for k in range(1, n_sim):
        pltpu.make_async_remote_copy(
            sums.at[me], sums.at[me], send_sem.at[0], sums_sem,
            device_id=(sec, sim_peer(k)), device_id_type=MESH,
        ).start()

    left64 = iota((width, 128), 1) < width

    def second(p, carry):
        hi, lo = [], []
        for h in range(2):
            n = jnp.clip(counts[2 * p + h] - base, 0, cells)
            rows = pl.ds(h * width, width)
            m = meanb[p, rows, :]
            m = jnp.concatenate([m] * (cells // 128), axis=1)
            c = jnp.where(lane_c < n, xv[p, rows, :] - m, 0.0)
            top = c.astype(BF16)
            hi.append(top)
            lo.append((c - top.astype(F32)).astype(BF16))
        hi = jnp.concatenate(hi, axis=0)
        lo = jnp.concatenate(lo, axis=0)
        both = dot_rows(hi, jnp.concatenate([hi, lo], axis=0))
        cross = both[:, 128:256]
        full = both[:, 0:128] + cross + cross.T
        cobuf[p] = jnp.where(left64, full[0:width, :], full[width:, :])
        return carry

    lax.fori_loop(0, pairs, second, 0)

    pltpu.make_async_copy(sums.at[pl.ds(0, n_sim - 1)], sums.at[pl.ds(0, n_sim - 1)], sums_sem).wait()
    total = sums[0]
    for d in range(1, n_sim):
        total = total + sums[d]
    means = total / n_all
    shift = mine / jnp.maximum(n_loc, 1.0) - means
    sq[...] = jnp.zeros((128, 128), F32)
    sq[0:pairs, :] = shift
    col_shift = sq[...].T
    row_shift = shift * n_loc

    qsum = jnp.zeros((width, 128), F32)
    per = half // chunks
    for p in range(pairs):
        i, pp = p // 2, p % 2
        c = jnp.where(left64, col_shift[0:width, p:p + 1], col_shift[width:, p:p + 1])
        co = cobuf[p] + c * row_shift[p:p + 1, :]
        qsum = qsum + co
        sendb[i, pl.ds(pp, width, stride=2), :] = co
        if pp == 1 and (i + 1) % per == 0:
            t = i // per
            for k in range(1, n_sim):
                to = sim_peer(k)
                pltpu.make_async_remote_copy(
                    sendb.at[pl.ds(t * per, per), pl.ds(pl.multiple_of(8 * to, 8), 8), :],
                    recvb.at[me, pl.ds(t * per, per)],
                    send_sem.at[1], piece_sem.at[t],
                    device_id=(sec, to), device_id_type=MESH,
                ).start()
    recvb[me] = sendb[:, pl.ds(pl.multiple_of(8 * me, 8), 8), :]

    swapped = pltpu.roll(means, width, 1)
    m_even = jnp.where(left16, means, swapped)
    m_odd = jnp.where(left16, swapped, means)
    cf_even, cf_odd = c_even.astype(F32), c_odd.astype(F32)

    def about(w_even, w_odd, least):
        count = jnp.sum(w_even, axis=0, keepdims=True) + jnp.sum(w_odd, axis=0, keepdims=True)
        weighted = jnp.sum(w_even * m_even, axis=0, keepdims=True) + jnp.sum(w_odd * m_odd, axis=0, keepdims=True)
        mean = weighted / jnp.maximum(count, least)
        d_even, d_odd = m_even - mean, m_odd - mean
        off = jnp.concatenate([d_even, d_odd], axis=0)
        left = jnp.concatenate([w_even * d_even, w_odd * d_odd], axis=0)
        return count, weighted, dot_high(left.T, off)[0:width, :]

    sec_count, sec_sum, sec_co = about(cf_even, cf_odd, 1.0)
    q = qsum + pltpu.roll(qsum, width, 1) + sec_co * (1.0 / n_sim)
    rows8 = jnp.where(sub8 == 0, sec_sum, jnp.where(sub8 == 1, sec_count, 0.0))
    for s in range(n_sec):
        qbuf[s, 0:8, :] = q[8 * s:8 * s + 8, :]
        qbuf[s, 8:16, :] = rows8
    for k in range(1, n_sec):
        to = sec_peer(k)
        pltpu.make_async_remote_copy(
            qbuf.at[to], qrecv.at[sec], send_sem.at[2], q_sem,
            device_id=(to, me), device_id_type=MESH,
        ).start()
    qrecv[sec] = qbuf[sec]

    turn[pl.ds(0, pairs, stride=2), :] = means
    turn[pl.ds(1, pairs, stride=2), :] = swapped
    mean_out[...] = turn[:, 0:width]
    grp_count, _, grp_co = about(
        jnp.where(o_even == me, cf_even, 0.0), jnp.where(o_odd == me, cf_odd, 0.0), 1.0
    )
    corrb[...] = grp_co
    left32 = iota((width // 2, 128), 1) < width
    between = jnp.where(left32, corrb[pl.ds(0, width // 2, stride=2), :], corrb[pl.ds(1, width // 2, stride=2), :])
    lane64, sub64 = iota((width, 128), 1), iota((width, 128), 0)
    names = jnp.where(
        ((sub64 % 8) // 2 == (lane64 % width) // n_sim) & (own64[...] == lane64 % n_sim), 1.0, 0.0
    ).T
    gsend[...] = jnp.zeros((8 * n_sim, 128), F32)

    pltpu.make_async_copy(qrecv.at[pl.ds(0, n_sec - 1)], qrecv.at[pl.ds(0, n_sec - 1)], q_sem).wait()
    part = qrecv[0, 0:8, :]
    sec_sums, sec_counts = qrecv[0, 8:9, :], qrecv[0, 9:10, :]
    sums_l, counts_l = [sec_sums], [sec_counts]
    for s in range(1, n_sec):
        part = part + qrecv[s, 0:8, :]
        sums_l.append(qrecv[s, 8:9, :])
        counts_l.append(qrecv[s, 9:10, :])
    sec_sums, sec_counts = jnp.concatenate(sums_l, axis=0), jnp.concatenate(counts_l, axis=0)
    zrecv[me] = part
    for k in range(1, n_sim):
        pltpu.make_async_remote_copy(
            zrecv.at[me], zrecv.at[me], send_sem.at[3], z_sem,
            device_id=(sec, sim_peer(k)), device_id_type=MESH,
        ).start()
    all_count = jnp.sum(sec_counts, axis=0, keepdims=True)
    all_mean = jnp.sum(sec_sums, axis=0, keepdims=True) / all_count
    gap = sec_sums / sec_counts - all_mean
    spread_co = dot_high((sec_counts * gap).T, gap)[0:width, :]
    gmean_out[...] = all_mean[:, 0:width]

    for t in range(chunks):
        pltpu.make_async_copy(
            recvb.at[pl.ds(0, n_sim - 1), pl.ds(0, per)], recvb.at[pl.ds(0, n_sim - 1), pl.ds(0, per)],
            piece_sem.at[t],
        ).wait()
    co = recvb[0]
    for d in range(1, n_sim):
        co = co + recvb[d]
    co = co.reshape(width, 128)
    named = dot_high(names, co)
    g = jnp.where(left64, named[0:width, :], named[width:, :])
    g = g + pltpu.roll(g, width, 1)
    gsend[pl.ds(0, n_sim, stride=8), :] = jnp.where(left16, g[0:16, :], g[16:32, :])
    gsend[pl.ds(1, n_sim, stride=8), :] = jnp.where(left16, g[32:48, :], g[48:64, :])
    mine8 = pl.ds(pl.multiple_of(8 * me, 8), 8)
    for k in range(1, n_sim):
        to = sim_peer(k)
        pltpu.make_async_remote_copy(
            gsend.at[pl.ds(pl.multiple_of(8 * to, 8), 8), :], grecv.at[mine8, :], send_sem.at[4], g_sem,
            device_id=(sec, to), device_id_type=MESH,
        ).start()
    grecv[mine8, :] = gsend[mine8, :]

    corrb[...] = co / (n64[...] - 1.0)
    for pp in range(2):
        for rr in range(2):
            a = corrb[pl.ds(4 * rr + pp, 8, stride=8), :]
            b = corrb[pl.ds(4 * rr + 2 + pp, 8, stride=8), :]
            turned = turn if rr == 0 else turn2
            turned[pl.ds(2 * pp, 8, stride=4), :] = jnp.where(left8, a, pltpu.roll(b, width, 1))
            turned[pl.ds(2 * pp + 1, 8, stride=4), :] = jnp.where(left8, pltpu.roll(a, width, 1), b)
    cov_out[:, 0:128] = turn[...]
    cov_out[:, 128:256] = turn2[...]

    pltpu.make_async_copy(zrecv.at[pl.ds(0, n_sim - 1)], zrecv.at[pl.ds(0, n_sim - 1)], z_sem).wait()
    part = zrecv[0]
    for d in range(1, n_sim):
        part = part + zrecv[d]
    frecv[sec] = part
    for k in range(1, n_sec):
        pltpu.make_async_remote_copy(
            frecv.at[sec], frecv.at[sec], send_sem.at[5], f_sem,
            device_id=(sec_peer(k), me), device_id_type=MESH,
        ).start()

    pltpu.make_async_copy(
        grecv.at[pl.ds(0, 8 * (n_sim - 1)), :], grecv.at[pl.ds(0, 8 * (n_sim - 1)), :], g_sem
    ).wait()
    grp[pl.ds(0, n_sim, stride=2), :] = grecv[pl.ds(0, n_sim, stride=8), :]
    grp[pl.ds(1, n_sim, stride=2), :] = grecv[pl.ds(1, n_sim, stride=8), :]
    grp_out[...] = (grp[...] + between) / jnp.maximum(grp_count - 1.0, 1.0)

    pltpu.make_async_copy(frecv.at[pl.ds(0, n_sec - 1)], frecv.at[pl.ds(0, n_sec - 1)], f_sem).wait()
    whole = frecv[...].reshape(width, 128)
    gcov_out[...] = ((whole + spread_co) / (all_count - 1.0))[:, 0:width]

    def sent(ref, n, sem):
        pltpu.make_async_copy(ref.at[pl.ds(0, n)], ref.at[pl.ds(0, n)], sem).wait()

    sent(sums, n_sim - 1, send_sem.at[0])
    sent(recvb, n_sim - 1, send_sem.at[1])
    sent(qrecv, n_sec - 1, send_sem.at[2])
    sent(zrecv, n_sim - 1, send_sem.at[3])
    sent(grecv, 8 * (n_sim - 1), send_sem.at[4])
    sent(frecv, n_sec - 1, send_sem.at[5])


def put(n, *refs):
    ins, outs, sem = refs[:n], refs[n:2 * n], refs[2 * n]
    copies = [pltpu.make_async_copy(a, b, sem.at[i]) for i, (a, b) in enumerate(zip(ins, outs))]
    for c in copies:
        c.start()
    for c in copies:
        c.wait()


def solution(mesh):
    n_sec, n_sim = mesh.shape["section"], mesh.shape["sim"]
    chunks = 2

    def local(state, owner, counts):
        slabs, width, cells = state.shape
        pairs = slabs // 2
        half = pairs // 2
        vmem = pl.BlockSpec(memory_space=pltpu.VMEM)
        smem = pl.BlockSpec(memory_space=pltpu.SMEM)
        dma = pltpu.SemaphoreType.DMA
        hbm = pl.BlockSpec(memory_space=pltpu.HBM)
        shapes = [
            jax.ShapeDtypeStruct((slabs, width), F32),
            jax.ShapeDtypeStruct((slabs, width * width // n_sim), F32),
            jax.ShapeDtypeStruct((width // 2, 2 * width), F32),
            jax.ShapeDtypeStruct((1, width), F32),
            jax.ShapeDtypeStruct((width, width), F32),
        ]
        found = pl.pallas_call(
            functools.partial(kernel, n_sec, n_sim, width, chunks),
            out_shape=shapes,
            in_specs=[hbm] * 3,
            out_specs=[vmem] * 5,
            scratch_shapes=[
                pltpu.VMEM((pairs, 2 * width, cells), F32),
                pltpu.VMEM((pairs, 2 * width, 128), F32),
                pltpu.VMEM((pairs, width, 128), F32),
                pltpu.VMEM((n_sim, pairs, 128), F32),
                pltpu.VMEM((128, 128), F32),
                pltpu.VMEM((half, 2 * width, 128), F32),
                pltpu.VMEM((n_sim, half, 8, 128), F32),
                pltpu.VMEM((n_sec, 16, 128), F32),
                pltpu.VMEM((n_sec, 16, 128), F32),
                pltpu.VMEM((n_sim, 8, 128), F32),
                pltpu.VMEM((n_sec, 8, 128), F32),
                pltpu.VMEM((8 * n_sim, 128), F32),
                pltpu.VMEM((8 * n_sim, 128), F32),
                pltpu.VMEM((width // 2, 128), F32),
                pltpu.VMEM((width, 128), F32),
                pltpu.VMEM((width, 128), F32),
                pltpu.VMEM((width, 128), jnp.int32),
                pltpu.VMEM((slabs, 128), F32),
                pltpu.VMEM((slabs, 128), F32),
                pltpu.SMEM((slabs,), jnp.int32),
                pltpu.SMEM((slabs,), jnp.int32),
                dma((pairs,)),
                dma((2,)),
                dma((6,)),
                dma(()),
                dma((chunks,)),
                dma(()),
                dma(()),
                dma(()),
                dma(()),
            ],
            compiler_params=pltpu.CompilerParams(
                collective_id=0, has_side_effects=True, vmem_limit_bytes=32 * 1024 * 1024
            ),
            name="moments",
        )(*(
            pltpu.with_memory_space_constraint(a, pltpu.HBM)
            for a in (state.reshape(pairs, 2 * width, cells), counts, owner.reshape(slabs))
        ))
        mean, cov, grp, gmean, gcov = pl.pallas_call(
            functools.partial(put, 5),
            out_shape=shapes,
            in_specs=[vmem] * 5,
            out_specs=[hbm] * 5,
            scratch_shapes=[dma((5,))],
            compiler_params=pltpu.CompilerParams(vmem_limit_bytes=4 * 1024 * 1024),
            name="put",
        )(*found)
        return mean, cov, grp.reshape(1, width * width), gmean.reshape(width), gcov

    return jax.shard_map(
        local,
        mesh=mesh,
        in_specs=(P("section", None, "sim"), P("section", None), P("section")),
        out_specs=(P("section", None), P("section", "sim"), P(("section", "sim"), None), P(), P()),
        check_vma=False,
    )
```

```python
import functools

import jax
import jax.numpy as jnp
from jax import lax
from jax.experimental import pallas as pl
from jax.experimental.pallas import tpu as pltpu
from jax.sharding import PartitionSpec as P

MESH = pl.DeviceIdType.MESH
HIGH = lax.Precision.HIGHEST
F32 = jnp.float32
BF16 = jnp.bfloat16


def dot_rows(a, b):
    return lax.dot_general(a, b, (((1,), (1,)), ((), ())), preferred_element_type=F32)


def dot_high(a, b):
    return jnp.dot(a, b, precision=HIGH, preferred_element_type=F32)


def iota(shape, dim):
    return lax.broadcasted_iota(jnp.int32, shape, dim)


def kernel(
    n_sec, n_sim, width, chunks,
    state, counts_hbm, owner_hbm,
    mean_out, cov_out, grp_out, gmean_out, gcov_out,
    xv, split, colsum, sums, sendb, recvb, qbuf, qrecv, zrecv, frecv, gsend, grecv, grp, corrb, n64, own64, turn, turn2,
    counts, owner, load_sem, int_sem, send_sem, sums_sem, piece_sem, q_sem, z_sem, f_sem, g_sem,
):
    pairs, _, cells = xv.shape
    half = pairs // 2
    sec = lax.axis_index("section")
    me = lax.axis_index("sim")
    z, x = me // 4, me % 4
    base = me * cells

    def sim_peer(k):
        return ((z + k // 4) % 4) * 4 + (x + k % 4) % 4

    def sec_peer(k):
        return (sec + k) % n_sec

    def block(i):
        return pl.ds(pl.multiple_of(8 * i, 8), 8)

    def double(i):
        return pl.ds(pl.multiple_of(16 * i, 16), 16)

    def arrived(ref, n, sem):
        pltpu.make_async_copy(ref.at[pl.ds(0, n)], ref.at[pl.ds(0, n)], sem).wait()

    small = [
        pltpu.make_async_copy(counts_hbm, counts, int_sem.at[0]),
        pltpu.make_async_copy(owner_hbm, owner, int_sem.at[1]),
    ]
    loads = {
        p: pltpu.make_async_copy(state.at[p], xv.at[p], load_sem.at[p])
        for i in range(half) for p in (i, i + half)
    }
    for c in small + list(loads.values()):
        c.start()

    barrier = pltpu.get_barrier_semaphore()
    for k in range(1, n_sim):
        pl.semaphore_signal(barrier, inc=1, device_id=(sec, sim_peer(k)), device_id_type=MESH)
    for k in range(1, n_sec):
        pl.semaphore_signal(barrier, inc=1, device_id=(sec_peer(k), me), device_id_type=MESH)

    for c in small:
        c.wait()

    lane8, sub8 = iota((8, 128), 1), iota((8, 128), 0)
    left8, first8 = lane8 < width, sub8 % 2 == 0
    for i in range(half):
        def spread(ref):
            return jnp.where(
                left8,
                jnp.where(first8, ref[2 * i], ref[2 * (i + half)]),
                jnp.where(first8, ref[2 * i + 1], ref[2 * (i + half) + 1]),
            )
        n64[8 * i:8 * i + 8, :] = spread(counts).astype(F32)
        own64[8 * i:8 * i + 8, :] = spread(owner)
    lane16, sub16 = iota((pairs, 128), 1), iota((pairs, 128), 0)
    left16 = lane16 < width
    c_even = jnp.zeros((pairs, 128), jnp.int32)
    c_odd, o_even, o_odd = c_even, c_even, c_even
    for p in range(pairs):
        here = sub16 == p
        c_even = jnp.where(here, counts[2 * p], c_even)
        c_odd = jnp.where(here, counts[2 * p + 1], c_odd)
        o_even = jnp.where(here, owner[2 * p], o_even)
        o_odd = jnp.where(here, owner[2 * p + 1], o_odd)
    n_int = jnp.where(left16, c_even, c_odd)
    colsum[...] = jnp.zeros((128, 128), F32)
    gsend[...] = jnp.zeros((8 * n_sim, 128), F32)

    lane_c = iota((1, cells), 1)
    left64 = iota((width, 128), 1) < width

    def centre(i):
        for pp in range(2):
            p = i + half * pp
            loads[p].wait()
        for pp in range(2):
            p = i + half * pp
            for h in range(2):
                n = jnp.clip(counts[2 * p + h] - base, 0, cells)
                live = lane_c < n
                cell = xv[p, h * width:(h + 1) * width, :]
                s = jnp.sum(jnp.where(live, cell, 0.0), axis=1, keepdims=True)
                colsum[h * width:(h + 1) * width, p:p + 1] = s
                m = s / jnp.maximum(n, 1).astype(F32)
                c = jnp.where(live, cell - m, 0.0)
                top = c.astype(BF16)
                split[i % 2, pp, h * width:(h + 1) * width, :] = top
                split[i % 2, pp, (2 + h) * width:(3 + h) * width, :] = (c - top.astype(F32)).astype(BF16)

    def multiply(i, qsum):
        for pp in range(2):
            both = dot_rows(split[i % 2, pp, 0:2 * width, :], split[i % 2, pp])
            cross = both[:, 128:256]
            full = both[:, 0:128] + cross + cross.T
            co = jnp.where(left64, full[0:width, :], full[width:, :])
            qsum = qsum + co
            sendb[i, pl.ds(pp, width, stride=2), :] = co
        return qsum

    per = half // chunks
    qsum = jnp.zeros((width, 128), F32)
    for i in range(half + 1):
        if i < half:
            centre(i)
        if i > 0:
            qsum = multiply(i - 1, qsum)
        if i > 0 and i % per == 0:
            t = i // per - 1
            if t == 0:
                pl.semaphore_wait(barrier, n_sim - 1 + n_sec - 1)
            for k in range(1, n_sim):
                to = sim_peer(k)
                pltpu.make_async_remote_copy(
                    sendb.at[pl.ds(t * per, per), block(to), :],
                    recvb.at[me, pl.ds(t * per, per)],
                    send_sem.at[1], piece_sem.at[t],
                    device_id=(sec, to), device_id_type=MESH,
                ).start()
    mine = colsum[...].T[0:pairs, :]
    sums[me] = mine
    for k in range(1, n_sim):
        pltpu.make_async_remote_copy(
            sums.at[me], sums.at[me], send_sem.at[0], sums_sem,
            device_id=(sec, sim_peer(k)), device_id_type=MESH,
        ).start()
    recvb[me] = sendb[:, block(me), :]

    def both_sides(value):
        turned = pltpu.roll(value, width, 1)
        return jnp.where(left16, value, turned), jnp.where(left16, turned, value)

    def about(m_even, m_odd, w_even, w_odd):
        count = jnp.sum(w_even + w_odd, axis=0, keepdims=True)
        mean = jnp.sum(w_even * m_even + w_odd * m_odd, axis=0, keepdims=True) / jnp.maximum(count, 1.0)
        d_even, d_odd = m_even - mean, m_odd - mean
        off = jnp.concatenate([d_even, d_odd], axis=0)
        left = jnp.concatenate([w_even * d_even, w_odd * d_odd], axis=0)
        return count, mean, dot_high(left.T, off)[0:width, :]

    def here(c, d):
        return jnp.clip(c - d * cells, 0, cells).astype(F32)

    n_mine = here(n_int, me)
    l_even, l_odd = both_sides(mine / jnp.maximum(n_mine, 1.0))
    dev_count, dev_mean, dev_co = about(l_even, l_odd, here(c_even, me), here(c_odd, me))
    q = qsum + pltpu.roll(qsum, width, 1) + dev_co
    rows8 = jnp.where(sub8 == 0, dev_mean, jnp.where(sub8 == 1, dev_count, 0.0))
    for s in range(n_sec):
        qbuf[16 * s:16 * s + 8, :] = q[8 * s:8 * s + 8, :]
        qbuf[16 * s + 8:16 * s + 16, :] = rows8
    for k in range(1, n_sec):
        to = sec_peer(k)
        pltpu.make_async_remote_copy(
            qbuf.at[double(to), :], qrecv.at[double(sec), :], send_sem.at[2], q_sem,
            device_id=(to, me), device_id_type=MESH,
        ).start()
    qrecv[double(sec), :] = qbuf[double(sec), :]

    lane64, sub64 = iota((width, 128), 1), iota((width, 128), 0)
    names = jnp.where(
        ((sub64 % 8) // 2 == (lane64 % width) // n_sim) & (own64[...] == lane64 % n_sim), 1.0, 0.0
    ).T

    def merged(ref, n):
        part = ref[0:8, :]
        for s in range(1, n):
            part = part + ref[16 * s:16 * s + 8, :]
        means = ref[pl.ds(8, n, stride=16), :]
        weights = ref[pl.ds(9, n, stride=16), :]
        count = jnp.sum(weights, axis=0, keepdims=True)
        mean = jnp.sum(weights * means, axis=0, keepdims=True) / jnp.maximum(count, 1.0)
        gap = means - mean
        corrb[...] = dot_high((weights * gap).T, gap)[0:width, :]
        return part + corrb[block(sec), :], mean, count

    arrived(qrecv, 16 * (n_sec - 1), q_sem)
    part, part_mean, part_count = merged(qrecv, n_sec)
    own_z = double(me)
    zrecv[own_z, :] = jnp.concatenate(
        [part, jnp.where(sub8 == 0, part_mean, jnp.where(sub8 == 1, part_count, 0.0))], axis=0
    )
    for k in range(1, n_sim):
        pltpu.make_async_remote_copy(
            zrecv.at[own_z, :], zrecv.at[own_z, :], send_sem.at[3], z_sem,
            device_id=(sec, sim_peer(k)), device_id_type=MESH,
        ).start()

    arrived(sums, n_sim - 1, sums_sem)
    total = sums[0]
    for d in range(1, n_sim):
        total = total + sums[d]
    means = total / n_int.astype(F32)
    turn[pl.ds(0, pairs, stride=2), :] = means
    turn[pl.ds(1, pairs, stride=2), :] = pltpu.roll(means, width, 1)
    mean_out[...] = turn[:, 0:width]

    rows = [jnp.zeros((pairs, 128), F32) for _ in range(4)]
    to_front = (128 - 4 * me) % 128
    for d in range(n_sim):
        n = here(n_int, d)
        gap = sums[d] / jnp.maximum(n, 1.0) - means
        front = pltpu.roll(gap, to_front, 1)
        gap_n = gap * n
        for r in range(4):
            rows[r] = rows[r] + jnp.where(left16, front[:, r:r + 1], front[:, width + r:width + r + 1]) * gap_n
    for r in range(4):
        for pp in range(2):
            corrb[pl.ds(2 * r + pp, half, stride=8), :] = rows[r][half * pp:half * (pp + 1), :]
    co = corrb[...]
    m_even, m_odd = both_sides(means)
    grp_count, _, grp_co = about(
        m_even, m_odd,
        jnp.where(o_even == me, c_even, 0).astype(F32), jnp.where(o_odd == me, c_odd, 0).astype(F32),
    )
    corrb[...] = grp_co
    left32 = iota((width // 2, 128), 1) < width
    between = jnp.where(left32, corrb[pl.ds(0, width // 2, stride=2), :], corrb[pl.ds(1, width // 2, stride=2), :])

    for t in range(chunks):
        few = recvb.at[pl.ds(0, n_sim - 1), pl.ds(0, per)]
        pltpu.make_async_copy(few, few, piece_sem.at[t]).wait()
    for d in range(n_sim):
        co = co + recvb[d].reshape(width, 128)
    named = dot_high(names, co)
    g = jnp.where(left64, named[0:width, :], named[width:, :])
    g = g + pltpu.roll(g, width, 1)
    gsend[pl.ds(0, n_sim, stride=8), :] = jnp.where(left16, g[0:16, :], g[16:32, :])
    gsend[pl.ds(1, n_sim, stride=8), :] = jnp.where(left16, g[32:48, :], g[48:64, :])
    for k in range(1, n_sim):
        to = sim_peer(k)
        pltpu.make_async_remote_copy(
            gsend.at[block(to), :], grecv.at[block(me), :], send_sem.at[4], g_sem,
            device_id=(sec, to), device_id_type=MESH,
        ).start()
    grecv[block(me), :] = gsend[block(me), :]

    arrived(zrecv, 16 * (n_sim - 1), z_sem)
    part, all_mean, all_count = merged(zrecv, n_sim)
    frecv[block(sec), :] = part
    for k in range(1, n_sec):
        pltpu.make_async_remote_copy(
            frecv.at[block(sec), :], frecv.at[block(sec), :], send_sem.at[5], f_sem,
            device_id=(sec_peer(k), me), device_id_type=MESH,
        ).start()
    gmean_out[...] = all_mean[:, 0:width]

    corrb[...] = co / (n64[...] - 1.0)
    for pp in range(2):
        for rr in range(2):
            a = corrb[pl.ds(4 * rr + pp, half, stride=8), :]
            b = corrb[pl.ds(4 * rr + 2 + pp, half, stride=8), :]
            turned = turn if rr == 0 else turn2
            turned[pl.ds(pairs * pp, half, stride=2), :] = jnp.where(left8, a, pltpu.roll(b, width, 1))
            turned[pl.ds(pairs * pp + 1, half, stride=2), :] = jnp.where(left8, pltpu.roll(a, width, 1), b)
    cov_out[:, 0:128] = turn[...]
    cov_out[:, 128:256] = turn2[...]

    arrived(grecv, 8 * (n_sim - 1), g_sem)
    grp[pl.ds(0, n_sim, stride=2), :] = grecv[pl.ds(0, n_sim, stride=8), :]
    grp[pl.ds(1, n_sim, stride=2), :] = grecv[pl.ds(1, n_sim, stride=8), :]
    grp_out[...] = (grp[...] + between) / jnp.maximum(grp_count - 1.0, 1.0)

    arrived(frecv, 8 * (n_sec - 1), f_sem)
    gcov_out[...] = (frecv[...] / (all_count - 1.0))[:, 0:width]

    arrived(sums, n_sim - 1, send_sem.at[0])
    arrived(recvb, n_sim - 1, send_sem.at[1])
    arrived(qrecv, 16 * (n_sec - 1), send_sem.at[2])
    arrived(zrecv, 16 * (n_sim - 1), send_sem.at[3])
    arrived(grecv, 8 * (n_sim - 1), send_sem.at[4])
    arrived(frecv, 8 * (n_sec - 1), send_sem.at[5])


def put(n, *refs):
    ins, outs, sem = refs[:n], refs[n:2 * n], refs[2 * n]
    copies = [pltpu.make_async_copy(a, b, sem.at[i]) for i, (a, b) in enumerate(zip(ins, outs))]
    for c in copies:
        c.start()
    for c in copies:
        c.wait()


def solution(mesh):
    n_sec, n_sim = mesh.shape["section"], mesh.shape["sim"]
    chunks = 4

    def local(state, owner, counts):
        slabs, width, cells = state.shape
        pairs = slabs // 2
        half = pairs // 2
        vmem = pl.BlockSpec(memory_space=pltpu.VMEM)
        smem = pl.BlockSpec(memory_space=pltpu.SMEM)
        dma = pltpu.SemaphoreType.DMA
        hbm = pl.BlockSpec(memory_space=pltpu.HBM)
        shapes = [
            jax.ShapeDtypeStruct((slabs, width), F32),
            jax.ShapeDtypeStruct((slabs, width * width // n_sim), F32),
            jax.ShapeDtypeStruct((width // 2, 2 * width), F32),
            jax.ShapeDtypeStruct((1, width), F32),
            jax.ShapeDtypeStruct((width, width), F32),
        ]
        found = pl.pallas_call(
            functools.partial(kernel, n_sec, n_sim, width, chunks),
            out_shape=shapes,
            in_specs=[hbm] * 3,
            out_specs=[vmem] * 5,
            scratch_shapes=[
                pltpu.VMEM((pairs, 2 * width, cells), F32),
                pltpu.VMEM((2, 2, 4 * width, cells), BF16),
                pltpu.VMEM((128, 128), F32),
                pltpu.VMEM((n_sim, pairs, 128), F32),
                pltpu.VMEM((half, 2 * width, 128), F32),
                pltpu.VMEM((n_sim, half, 8, 128), F32),
                pltpu.VMEM((16 * n_sec, 128), F32),
                pltpu.VMEM((16 * n_sec, 128), F32),
                pltpu.VMEM((16 * n_sim, 128), F32),
                pltpu.VMEM((8 * n_sec, 128), F32),
                pltpu.VMEM((8 * n_sim, 128), F32),
                pltpu.VMEM((8 * n_sim, 128), F32),
                pltpu.VMEM((width // 2, 128), F32),
                pltpu.VMEM((width, 128), F32),
                pltpu.VMEM((width, 128), F32),
                pltpu.VMEM((width, 128), jnp.int32),
                pltpu.VMEM((slabs, 128), F32),
                pltpu.VMEM((slabs, 128), F32),
                pltpu.SMEM((slabs,), jnp.int32),
                pltpu.SMEM((slabs,), jnp.int32),
                dma((pairs,)),
                dma((2,)),
                dma((6,)),
                dma(()),
                dma((chunks,)),
                dma(()),
                dma(()),
                dma(()),
                dma(()),
            ],
            compiler_params=pltpu.CompilerParams(
                collective_id=0, has_side_effects=True, vmem_limit_bytes=32 * 1024 * 1024
            ),
            name="moments",
        )(*(
            pltpu.with_memory_space_constraint(a, pltpu.HBM)
            for a in (state.reshape(pairs, 2 * width, cells), counts, owner.reshape(slabs))
        ))
        mean, cov, grp, gmean, gcov = pl.pallas_call(
            functools.partial(put, 5),
            out_shape=shapes,
            in_specs=[vmem] * 5,
            out_specs=[hbm] * 5,
            scratch_shapes=[dma((5,))],
            compiler_params=pltpu.CompilerParams(vmem_limit_bytes=4 * 1024 * 1024),
            name="put",
        )(*found)
        return mean, cov, grp.reshape(1, width * width), gmean.reshape(width), gcov

    return jax.shard_map(
        local,
        mesh=mesh,
        in_specs=(P("section", None, "sim"), P("section", None), P("section")),
        out_specs=(P("section", None), P("section", "sim"), P(("section", "sim"), None), P(), P()),
        check_vma=False,
    )
```

```python
import functools

import jax
import jax.numpy as jnp
from jax import lax
from jax.experimental import pallas as pl
from jax.experimental.pallas import tpu as pltpu
from jax.sharding import PartitionSpec as P

MESH = pl.DeviceIdType.MESH
F32 = jnp.float32
BF16 = jnp.bfloat16


def dot_rows(a, b):
    return lax.dot_general(a, b, (((1,), (1,)), ((), ())), preferred_element_type=F32)


def outer_sum(a, b):
    a_top, b_top = a.astype(BF16).astype(F32), b.astype(BF16).astype(F32)
    left = jnp.concatenate([a_top, a - a_top, a_top], axis=0)
    right = jnp.concatenate([b_top, b_top, b - b_top], axis=0)
    return jnp.dot(left.T.astype(BF16), right.astype(BF16), preferred_element_type=F32)


def iota(shape, dim):
    return lax.broadcasted_iota(jnp.int32, shape, dim)


def kernel(
    n_sec, n_sim, width,
    state, counts_hbm, owner_hbm,
    mean_out, cov_out, grp_out, gmean_out, gcov_out,
    xv, split, colsum, sums, sendb, first_x, first_z, part_x, part_z, second_x, second_z, straight, sel, gaps, fold, qrecv, zrecv, gsend, grecv, grp, corrb, n64, own64, turn, turn2,
    counts, owner, load_sem, int_sem, send_sem, sums_sem, first_sem, second_sem, straight_sem, q_sem, z_sem, g_sem,
):
    pairs, _, cells = xv.shape
    half = pairs // 2
    sec = lax.axis_index("section")
    me = lax.axis_index("sim")
    z, x = me // 4, me % 4
    base = me * cells

    def sim_peer(k):
        return ((z + k // 4) % 4) * 4 + (x + k % 4) % 4

    def sec_peer(k):
        return (sec + k) % n_sec

    def block(i):
        return pl.ds(pl.multiple_of(8 * i, 8), 8)

    def along_x(k):
        return (x + k) % 4

    def along_z(k):
        return (z + k) % 4

    def arrived(ref, n, sem):
        pltpu.make_async_copy(ref.at[pl.ds(0, n)], ref.at[pl.ds(0, n)], sem).wait()

    small = [
        pltpu.make_async_copy(counts_hbm, counts, int_sem.at[0]),
        pltpu.make_async_copy(owner_hbm, owner, int_sem.at[1]),
    ]
    loads = {
        p: pltpu.make_async_copy(state.at[p], xv.at[p], load_sem.at[p])
        for i in range(half) for p in (i, i + half)
    }
    for c in small + list(loads.values()):
        c.start()

    barrier = pltpu.get_barrier_semaphore()
    for k in range(1, n_sim):
        pl.semaphore_signal(barrier, inc=1, device_id=(sec, sim_peer(k)), device_id_type=MESH)
    for k in range(1, n_sec):
        pl.semaphore_signal(barrier, inc=1, device_id=(sec_peer(k), me), device_id_type=MESH)

    for c in small:
        c.wait()

    lane8, sub8 = iota((8, 128), 1), iota((8, 128), 0)
    left8, first8 = lane8 < width, sub8 % 2 == 0
    for i in range(half):
        def spread(ref):
            return jnp.where(
                left8,
                jnp.where(first8, ref[2 * i], ref[2 * (i + half)]),
                jnp.where(first8, ref[2 * i + 1], ref[2 * (i + half) + 1]),
            )
        n64[8 * i:8 * i + 8, :] = spread(counts).astype(F32)
        own64[8 * i:8 * i + 8, :] = spread(owner)
    lane16, sub16 = iota((pairs, 128), 1), iota((pairs, 128), 0)
    left16 = lane16 < width
    c_even = jnp.zeros((pairs, 128), jnp.int32)
    c_odd, o_even, o_odd = c_even, c_even, c_even
    for p in range(pairs):
        here = sub16 == p
        c_even = jnp.where(here, counts[2 * p], c_even)
        c_odd = jnp.where(here, counts[2 * p + 1], c_odd)
        o_even = jnp.where(here, owner[2 * p], o_even)
        o_odd = jnp.where(here, owner[2 * p + 1], o_odd)
    n_int = jnp.where(left16, c_even, c_odd)
    colsum[...] = jnp.zeros((128, 128), F32)
    row128, col128 = iota((128, 128), 0), iota((128, 128), 1)
    for r in range(4):
        sel[:, 128 * r:128 * (r + 1)] = jnp.where(
            row128 == (col128 // width) * width + 4 * me + r, 1.0, 0.0
        ).astype(BF16)
    gsend[...] = jnp.zeros((8 * n_sim, 128), F32)

    lane_c = iota((1, cells), 1)
    left64 = iota((width, 128), 1) < width

    def centre(i):
        for pp in range(2):
            p = i + half * pp
            loads[p].wait()
        for pp in range(2):
            p = i + half * pp
            for h in range(2):
                n = jnp.clip(counts[2 * p + h] - base, 0, cells)
                live = lane_c < n
                for r in range(h * width, (h + 1) * width, 16):
                    cell = xv[p, r:r + 16, :]
                    s = jnp.sum(jnp.where(live, cell, 0.0), axis=1, keepdims=True)
                    colsum[r:r + 16, p:p + 1] = s
                    m = s / jnp.maximum(n, 1).astype(F32)
                    c = jnp.where(live, cell - m, 0.0)
                    top = c.astype(BF16)
                    split[i % 2, pp, r:r + 16, :] = top
                    split[i % 2, pp, 2 * width + r:2 * width + r + 16, :] = (c - top.astype(F32)).astype(BF16)

    def multiply(i, qsum):
        for pp in range(2):
            both = dot_rows(split[i % 2, pp], split[i % 2, pp, 0:2 * width, :])
            cross = both[2 * width:, :]
            full = both[0:2 * width, :] + cross + cross.T
            co = jnp.where(left64, full[0:width, :], full[width:, :])
            qsum = qsum + co
            for j in range(4):
                sendb[i, j, pl.ds(pp, width // 4, stride=2), :] = co[width // 4 * j:width // 4 * (j + 1), :]
        return qsum

    staged = first_x.shape[1]
    qsum = jnp.zeros((width, 128), F32)
    for i in range(half + 1):
        if i < half:
            centre(i)
        if i > 0:
            qsum = multiply(i - 1, qsum)
        if i > 0 and i % 2 == 0:
            t = i // 2 - 1
            if t == 0:
                pl.semaphore_wait(barrier, n_sim - 1 + n_sec - 1)
            if t < staged:
                for k in range(1, 4):
                    to = along_x(k)
                    pltpu.make_async_remote_copy(
                        sendb.at[i - 2, :, block(to), :], first_x.at[k - 1, t], send_sem.at[1], first_sem.at[t, 0],
                        device_id=(sec, z * 4 + to), device_id_type=MESH,
                    ).start()
                    to = along_z(k)
                    pltpu.make_async_remote_copy(
                        sendb.at[i - 1, to], first_z.at[k - 1, t], send_sem.at[7], first_sem.at[t, 1],
                        device_id=(sec, to * 4 + x), device_id_type=MESH,
                    ).start()
            else:
                for k in range(1, n_sim):
                    pltpu.make_async_remote_copy(
                        sendb.at[pl.ds(i - 2, 2), along_z(k // 4), block(along_x(k % 4)), :],
                        straight.at[k - 1, t - staged],
                        send_sem.at[5], straight_sem.at[t - staged],
                        device_id=(sec, sim_peer(k)), device_id_type=MESH,
                    ).start()
    mine = colsum[...].T[0:pairs, :]
    sums[me] = mine
    for k in range(1, n_sim):
        pltpu.make_async_remote_copy(
            sums.at[me], sums.at[me], send_sem.at[0], sums_sem,
            device_id=(sec, sim_peer(k)), device_id_type=MESH,
        ).start()

    def both_sides(value):
        turned = pltpu.roll(value, width, 1)
        return jnp.where(left16, value, turned), jnp.where(left16, turned, value)

    def about(m_even, m_odd, w_even, w_odd):
        count = jnp.sum(w_even + w_odd, axis=0, keepdims=True)
        mean = jnp.sum(w_even * m_even + w_odd * m_odd, axis=0, keepdims=True) / jnp.maximum(count, 1.0)
        d_even, d_odd = m_even - mean, m_odd - mean
        off = jnp.concatenate([d_even, d_odd], axis=0)
        left = jnp.concatenate([w_even * d_even, w_odd * d_odd], axis=0)
        return count, mean, outer_sum(left, off)[0:width, :]

    def here(c, d):
        return jnp.clip(c - d * cells, 0, cells).astype(F32)

    n_mine = here(n_int, me)
    l_even, l_odd = both_sides(mine / jnp.maximum(n_mine, 1.0))
    dev_count, dev_mean, dev_co = about(l_even, l_odd, here(c_even, me), here(c_odd, me))
    q = qsum + pltpu.roll(qsum, width, 1) + dev_co

    lane32, sub32 = iota((width // 2, 128), 1), iota((width // 2, 128), 0)
    left32 = lane32 < width
    col32 = lane32 % width
    inner32 = col32 < width // 2
    above32 = col32 > sub32

    def folded(m, mean, count):
        top, bottom = m[0:width // 2, :], m[width // 2:width, :]
        kept = jnp.where(inner32 & ~above32, pltpu.roll(bottom, width // 2, 1), top)
        diagonal = jnp.sum(jnp.where(col32 == sub32, top, 0.0), axis=0, keepdims=True)
        info = jnp.where(sub8 == 0, mean, jnp.where(sub8 == 1, count, jnp.where(sub8 == 2, diagonal, 0.0)))
        quarter = width // 4
        return jnp.concatenate(
            [jnp.where(left16, kept[0:quarter, :], kept[quarter:2 * quarter, :]), info], axis=0
        )

    def unfolded(m):
        swapped = pltpu.roll(m[0:pairs, :], width, 1)
        kept = jnp.concatenate(
            [jnp.where(left16, m[0:pairs, :], swapped), jnp.where(left16, swapped, m[0:pairs, :])], axis=0
        )
        turned = jnp.concatenate([kept, kept, kept, kept], axis=0).T[0:width, :]
        first = jnp.where(above32, kept, jnp.where(col32 == sub32, m[pairs + 2:pairs + 3, :], turned[0:width // 2, :]))
        top = jnp.where(inner32, first, kept)
        last = pltpu.roll(jnp.where(above32, turned[0:width // 2, :], kept), width // 2, 1)
        bottom = jnp.where(inner32, turned[width // 2:, :], last)
        return jnp.concatenate([top, bottom], axis=0)

    def third(i):
        return pl.ds(pl.multiple_of(24 * i, 8), 24)

    fold[...] = folded(q, dev_mean, dev_count)
    for k in range(1, n_sec):
        pltpu.make_async_remote_copy(
            fold, qrecv.at[third(sec), :], send_sem.at[2], q_sem,
            device_id=(sec_peer(k), me), device_id_type=MESH,
        ).start()
    qrecv[third(sec), :] = fold[...]

    lane64, sub64 = iota((width, 128), 1), iota((width, 128), 0)
    names = jnp.where(
        ((sub64 % 8) // 2 == (lane64 % width) // n_sim) & (own64[...] == lane64 % n_sim), 1.0, 0.0
    )
    names = jnp.concatenate([names, names], axis=0).T.astype(BF16)

    def merged(ref, n):
        part = ref[0:24, :]
        for s in range(1, n):
            part = part + ref[24 * s:24 * (s + 1), :]
        means = ref[pl.ds(pairs, n, stride=24), :]
        weights = ref[pl.ds(pairs + 1, n, stride=24), :]
        count = jnp.sum(weights, axis=0, keepdims=True)
        mean = jnp.sum(weights * means, axis=0, keepdims=True) / jnp.maximum(count, 1.0)
        gap = means - mean
        return part, mean, count, outer_sum(weights * gap, gap)[0:width, :]

    for t in range(staged):
        few = first_x.at[:, t]
        pltpu.make_async_copy(few, few, first_sem.at[t, 0]).wait()
        few = first_z.at[:, t]
        pltpu.make_async_copy(few, few, first_sem.at[t, 1]).wait()
        part_x[t] = sendb[2 * t, :, block(x), :] + first_x[0, t] + first_x[1, t] + first_x[2, t]
        part_z[t] = sendb[2 * t + 1, z] + first_z[0, t] + first_z[1, t] + first_z[2, t]
    for k in range(1, 4):
        to = along_z(k)
        pltpu.make_async_remote_copy(
            part_x.at[:, to], second_x.at[k - 1], send_sem.at[6], second_sem.at[0],
            device_id=(sec, to * 4 + x), device_id_type=MESH,
        ).start()
        to = along_x(k)
        pltpu.make_async_remote_copy(
            part_z.at[:, block(to), :], second_z.at[k - 1], send_sem.at[8], second_sem.at[1],
            device_id=(sec, z * 4 + to), device_id_type=MESH,
        ).start()

    arrived(qrecv, 24 * (n_sec - 1), q_sem)
    part, part_mean, part_count, part_co = merged(qrecv, n_sec)
    extra = folded(part_co, part_mean, part_count)
    info = jnp.where(sub8 == 2, part[pairs:, :] + extra[pairs:, :], extra[pairs:, :])
    zrecv[third(me), :] = jnp.concatenate([part[0:pairs, :] + extra[0:pairs, :], info], axis=0)
    for k in range(1, n_sim):
        pltpu.make_async_remote_copy(
            zrecv.at[third(me), :], zrecv.at[third(me), :], send_sem.at[3], z_sem,
            device_id=(sec, sim_peer(k)), device_id_type=MESH,
        ).start()

    arrived(sums, n_sim - 1, sums_sem)
    total = sums[0]
    for d in range(1, n_sim):
        total = total + sums[d]
    means = total / n_int.astype(F32)
    turn[pl.ds(0, pairs, stride=2), :] = means
    turn[pl.ds(1, pairs, stride=2), :] = pltpu.roll(means, width, 1)
    mean_out[...] = turn[:, 0:width]

    weighted = []
    for d in range(n_sim):
        n = here(n_int, d)
        gap = sums[d] / jnp.maximum(n, 1.0) - means
        weighted.append(gap * n)
        top = gap.astype(BF16)
        gaps[pairs * d:pairs * (d + 1), :] = top
        gaps[pairs * (n_sim + d):pairs * (n_sim + d + 1), :] = (gap - top.astype(F32)).astype(BF16)
    for r in range(4):
        picked = jnp.dot(gaps[...], sel[:, 128 * r:128 * (r + 1)], preferred_element_type=F32)
        rows = jnp.zeros((pairs, 128), F32)
        for d in range(n_sim):
            one = picked[pairs * d:pairs * (d + 1), :] + picked[pairs * (n_sim + d):pairs * (n_sim + d + 1), :]
            rows = rows + one * weighted[d]
        for pp in range(2):
            corrb[pl.ds(2 * r + pp, half, stride=8), :] = rows[half * pp:half * (pp + 1), :]
    co = corrb[...]
    m_even, m_odd = both_sides(means)
    grp_count, _, grp_co = about(
        m_even, m_odd,
        jnp.where(o_even == me, c_even, 0).astype(F32), jnp.where(o_odd == me, c_odd, 0).astype(F32),
    )
    corrb[...] = grp_co
    between = jnp.where(left32, corrb[pl.ds(0, width // 2, stride=2), :], corrb[pl.ds(1, width // 2, stride=2), :])

    pltpu.make_async_copy(second_x, second_x, second_sem.at[0]).wait()
    pltpu.make_async_copy(second_z, second_z, second_sem.at[1]).wait()
    tiles = []
    for t in range(staged):
        tiles.append(part_x[t, z] + second_x[0, t] + second_x[1, t] + second_x[2, t])
        tiles.append(part_z[t, block(x), :] + second_z[0, t] + second_z[1, t] + second_z[2, t])
    for t in range(half // 2 - staged):
        few = straight.at[:, t]
        pltpu.make_async_copy(few, few, straight_sem.at[t]).wait()
        for u in range(2):
            tile = sendb[2 * (staged + t) + u, z, block(x), :]
            for k in range(n_sim - 1):
                tile = tile + straight[k, t, u]
            tiles.append(tile)
    co = co + jnp.concatenate(tiles, axis=0)
    top = co.astype(BF16)
    low = (co - top.astype(F32)).astype(BF16)
    named = jnp.dot(names, jnp.concatenate([top, low], axis=0), preferred_element_type=F32)
    g = jnp.where(left64, named[0:width, :], named[width:, :])
    g = g + pltpu.roll(g, width, 1)
    gsend[pl.ds(0, n_sim, stride=8), :] = jnp.where(left16, g[0:16, :], g[16:32, :])
    gsend[pl.ds(1, n_sim, stride=8), :] = jnp.where(left16, g[32:48, :], g[48:64, :])
    for k in range(1, n_sim):
        to = sim_peer(k)
        pltpu.make_async_remote_copy(
            gsend.at[block(to), :], grecv.at[block(me), :], send_sem.at[4], g_sem,
            device_id=(sec, to), device_id_type=MESH,
        ).start()
    grecv[block(me), :] = gsend[block(me), :]

    arrived(zrecv, 24 * (n_sim - 1), z_sem)
    part, all_mean, all_count, all_co = merged(zrecv, n_sim)
    gmean_out[...] = all_mean[:, 0:width]
    gcov_out[...] = ((unfolded(part) + all_co) / (all_count - 1.0))[:, 0:width]

    corrb[...] = co / (n64[...] - 1.0)
    for pp in range(2):
        for rr in range(2):
            a = corrb[pl.ds(4 * rr + pp, half, stride=8), :]
            b = corrb[pl.ds(4 * rr + 2 + pp, half, stride=8), :]
            turned = turn if rr == 0 else turn2
            turned[pl.ds(pairs * pp, half, stride=2), :] = jnp.where(left8, a, pltpu.roll(b, width, 1))
            turned[pl.ds(pairs * pp + 1, half, stride=2), :] = jnp.where(left8, pltpu.roll(a, width, 1), b)
    cov_out[:, 0:128] = turn[...]
    cov_out[:, 128:256] = turn2[...]

    arrived(grecv, 8 * (n_sim - 1), g_sem)
    grp[pl.ds(0, n_sim, stride=2), :] = grecv[pl.ds(0, n_sim, stride=8), :]
    grp[pl.ds(1, n_sim, stride=2), :] = grecv[pl.ds(1, n_sim, stride=8), :]
    grp_out[...] = (grp[...] + between) / jnp.maximum(grp_count - 1.0, 1.0)

    arrived(sums, n_sim - 1, send_sem.at[0])
    arrived(first_x, 3, send_sem.at[1])
    arrived(first_z, 3, send_sem.at[7])
    arrived(qrecv, 24 * (n_sec - 1), send_sem.at[2])
    arrived(zrecv, 24 * (n_sim - 1), send_sem.at[3])
    arrived(grecv, 8 * (n_sim - 1), send_sem.at[4])
    arrived(straight, n_sim - 1, send_sem.at[5])
    arrived(second_x, 3, send_sem.at[6])
    arrived(second_z, 3, send_sem.at[8])


def put(n, *refs):
    ins, outs, sem = refs[:n], refs[n:2 * n], refs[2 * n]
    copies = [pltpu.make_async_copy(a, b, sem.at[i]) for i, (a, b) in enumerate(zip(ins, outs))]
    for c in copies:
        c.start()
    for c in copies:
        c.wait()


def solution(mesh):
    n_sec, n_sim = mesh.shape["section"], mesh.shape["sim"]

    def local(state, owner, counts):
        slabs, width, cells = state.shape
        pairs = slabs // 2
        half = pairs // 2
        staged = 2
        vmem = pl.BlockSpec(memory_space=pltpu.VMEM)
        smem = pl.BlockSpec(memory_space=pltpu.SMEM)
        dma = pltpu.SemaphoreType.DMA
        hbm = pl.BlockSpec(memory_space=pltpu.HBM)
        shapes = [
            jax.ShapeDtypeStruct((slabs, width), F32),
            jax.ShapeDtypeStruct((slabs, width * width // n_sim), F32),
            jax.ShapeDtypeStruct((width // 2, 2 * width), F32),
            jax.ShapeDtypeStruct((1, width), F32),
            jax.ShapeDtypeStruct((width, width), F32),
        ]
        found = pl.pallas_call(
            functools.partial(kernel, n_sec, n_sim, width),
            out_shape=shapes,
            in_specs=[hbm] * 3,
            out_specs=[vmem] * 5,
            scratch_shapes=[
                pltpu.VMEM((pairs, 2 * width, cells), F32),
                pltpu.VMEM((2, 2, 4 * width, cells), BF16),
                pltpu.VMEM((128, 128), F32),
                pltpu.VMEM((n_sim, pairs, 128), F32),
                pltpu.VMEM((half, 4, 32, 128), F32),
                pltpu.VMEM((3, staged, 4, 8, 128), F32),
                pltpu.VMEM((3, staged, 32, 128), F32),
                pltpu.VMEM((staged, 4, 8, 128), F32),
                pltpu.VMEM((staged, 32, 128), F32),
                pltpu.VMEM((3, staged, 8, 128), F32),
                pltpu.VMEM((3, staged, 8, 128), F32),
                pltpu.VMEM((n_sim - 1, half // 2 - staged, 2, 8, 128), F32),
                pltpu.VMEM((128, 512), BF16),
                pltpu.VMEM((2 * n_sim * pairs, 128), BF16),
                pltpu.VMEM((24, 128), F32),
                pltpu.VMEM((24 * n_sec, 128), F32),
                pltpu.VMEM((24 * n_sim, 128), F32),
                pltpu.VMEM((8 * n_sim, 128), F32),
                pltpu.VMEM((8 * n_sim, 128), F32),
                pltpu.VMEM((width // 2, 128), F32),
                pltpu.VMEM((width, 128), F32),
                pltpu.VMEM((width, 128), F32),
                pltpu.VMEM((width, 128), jnp.int32),
                pltpu.VMEM((slabs, 128), F32),
                pltpu.VMEM((slabs, 128), F32),
                pltpu.SMEM((slabs,), jnp.int32),
                pltpu.SMEM((slabs,), jnp.int32),
                dma((pairs,)),
                dma((2,)),
                dma((9,)),
                dma(()),
                dma((staged, 2)),
                dma((2,)),
                dma((half // 2 - staged,)),
                dma(()),
                dma(()),
                dma(()),
            ],
            compiler_params=pltpu.CompilerParams(
                collective_id=0, has_side_effects=True, vmem_limit_bytes=32 * 1024 * 1024
            ),
            name="moments",
        )(*(
            pltpu.with_memory_space_constraint(a, pltpu.HBM)
            for a in (state.reshape(pairs, 2 * width, cells), counts, owner.reshape(slabs))
        ))
        mean, cov, grp, gmean, gcov = pl.pallas_call(
            functools.partial(put, 5),
            out_shape=shapes,
            in_specs=[vmem] * 5,
            out_specs=[hbm] * 5,
            scratch_shapes=[dma((5,))],
            compiler_params=pltpu.CompilerParams(vmem_limit_bytes=4 * 1024 * 1024),
            name="put",
        )(*found)
        return mean, cov, grp.reshape(1, width * width), gmean.reshape(width), gcov

    return jax.shard_map(
        local,
        mesh=mesh,
        in_specs=(P("section", None, "sim"), P("section", None), P("section")),
        out_specs=(P("section", None), P("section", "sim"), P(("section", "sim"), None), P(), P()),
        check_vma=False,
    )
```

```python
import functools

import jax
import jax.numpy as jnp
from jax import lax
from jax.experimental import pallas as pl
from jax.experimental.pallas import tpu as pltpu
from jax.sharding import PartitionSpec as P

MESH = pl.DeviceIdType.MESH
F32 = jnp.float32
BF16 = jnp.bfloat16


def dot_rows(a, b):
    return lax.dot_general(a, b, (((1,), (1,)), ((), ())), preferred_element_type=F32)


def outer_sum(a, b):
    a_top, b_top = a.astype(BF16).astype(F32), b.astype(BF16).astype(F32)
    left = jnp.concatenate([a_top, a - a_top, a_top], axis=0)
    right = jnp.concatenate([b_top, b_top, b - b_top], axis=0)
    return jnp.dot(left.T.astype(BF16), right.astype(BF16), preferred_element_type=F32)


def iota(shape, dim):
    return lax.broadcasted_iota(jnp.int32, shape, dim)


def kernel(
    n_sec, n_sim, width,
    state, counts_hbm, owner_hbm,
    mean_out, cov_out, grp_out, gmean_out, gcov_out,
    xv, split, colsum, sums, sendb, first_x, first_z, part_x, part_z, second_x, second_z, straight, sel, gaps, fold, qrecv, zrecv, gsend, grecv, grp, corrb, n64, own64, turn, turn2,
    counts, owner, load_sem, int_sem, send_sem, sums_sem, first_sem, second_sem, straight_sem, q_sem, z_sem, g_sem,
):
    pairs, _, cells = xv.shape
    half = pairs // 2
    sec = lax.axis_index("section")
    me = lax.axis_index("sim")
    z, x = me // 4, me % 4
    base = me * cells

    def sim_peer(k):
        return ((z + k // 4) % 4) * 4 + (x + k % 4) % 4

    def sec_peer(k):
        return (sec + k) % n_sec

    def block(i):
        return pl.ds(pl.multiple_of(8 * i, 8), 8)

    def along_x(k):
        return (x + k) % 4

    def along_z(k):
        return (z + k) % 4

    def arrived(ref, n, sem):
        pltpu.make_async_copy(ref.at[pl.ds(0, n)], ref.at[pl.ds(0, n)], sem).wait()

    small = [
        pltpu.make_async_copy(counts_hbm, counts, int_sem.at[0]),
        pltpu.make_async_copy(owner_hbm, owner, int_sem.at[1]),
    ]
    loads = {
        p: pltpu.make_async_copy(state.at[p], xv.at[p], load_sem.at[p])
        for i in range(half) for p in (i, i + half)
    }
    for c in small + list(loads.values()):
        c.start()

    barrier = pltpu.get_barrier_semaphore()
    for k in range(1, n_sim):
        pl.semaphore_signal(barrier, inc=1, device_id=(sec, sim_peer(k)), device_id_type=MESH)
    for k in range(1, n_sec):
        pl.semaphore_signal(barrier, inc=1, device_id=(sec_peer(k), me), device_id_type=MESH)

    for c in small:
        c.wait()

    lane8, sub8 = iota((8, 128), 1), iota((8, 128), 0)
    left8, first8 = lane8 < width, sub8 % 2 == 0
    for i in range(half):
        def spread(ref):
            return jnp.where(
                left8,
                jnp.where(first8, ref[2 * i], ref[2 * (i + half)]),
                jnp.where(first8, ref[2 * i + 1], ref[2 * (i + half) + 1]),
            )
        n64[8 * i:8 * i + 8, :] = spread(counts).astype(F32)
        own64[8 * i:8 * i + 8, :] = spread(owner)
    lane16, sub16 = iota((pairs, 128), 1), iota((pairs, 128), 0)
    left16 = lane16 < width
    c_even = jnp.zeros((pairs, 128), jnp.int32)
    c_odd, o_even, o_odd = c_even, c_even, c_even
    for p in range(pairs):
        here = sub16 == p
        c_even = jnp.where(here, counts[2 * p], c_even)
        c_odd = jnp.where(here, counts[2 * p + 1], c_odd)
        o_even = jnp.where(here, owner[2 * p], o_even)
        o_odd = jnp.where(here, owner[2 * p + 1], o_odd)
    n_int = jnp.where(left16, c_even, c_odd)
    colsum[...] = jnp.zeros((128, 128), F32)
    row128, col128 = iota((128, 128), 0), iota((128, 128), 1)
    for r in range(4):
        sel[:, 128 * r:128 * (r + 1)] = jnp.where(
            row128 == (col128 // width) * width + 4 * me + r, 1.0, 0.0
        ).astype(BF16)
    gsend[...] = jnp.zeros((8 * n_sim, 128), F32)

    lane_c = iota((1, cells), 1)
    left64 = iota((width, 128), 1) < width

    def centre(i):
        for pp in range(2):
            p = i + half * pp
            for h in range(2):
                n = jnp.clip(counts[2 * p + h] - base, 0, cells)
                live = lane_c < n
                for r in range(h * width, (h + 1) * width, 16):
                    cell = xv[p, r:r + 16, :]
                    s = jnp.sum(jnp.where(live, cell, 0.0), axis=1, keepdims=True)
                    colsum[r:r + 16, p:p + 1] = s
                    m = s / jnp.maximum(n, 1).astype(F32)
                    c = jnp.where(live, cell - m, 0.0)
                    top = c.astype(BF16)
                    split[i % 2, pp, r:r + 16, :] = top
                    split[i % 2, pp, 2 * width + r:2 * width + r + 16, :] = (c - top.astype(F32)).astype(BF16)

    def multiply(i, qsum):
        for pp in range(2):
            terms = split[i % 2, pp]
            both = dot_rows(terms, terms)
            full = both[0:2 * width, :] + both[2 * width:, :]
            full = full[:, 0:2 * width] + full[:, 2 * width:]
            co = jnp.where(left64, full[0:width, :], full[width:, :])
            qsum = qsum + co
            for j in range(4):
                sendb[i, j, pl.ds(pp, width // 4, stride=2), :] = co[width // 4 * j:width // 4 * (j + 1), :]
        return qsum

    staged = first_x.shape[1]
    qsum = jnp.zeros((width, 128), F32)
    for i in range(half + 1):
        if i == 0 or i % 2 == 1:
            for p in range(i, min(half, i + 1 + i % 2)):
                loads[p].wait()
                loads[p + half].wait()
        if i < half:
            centre(i)
        if i > 0:
            qsum = multiply(i - 1, qsum)
        if i == half - 1:
            mine = colsum[...].T[0:pairs, :]
            sums[me] = mine
            for k in range(1, n_sim):
                pltpu.make_async_remote_copy(
                    sums.at[me], sums.at[me], send_sem.at[0], sums_sem,
                    device_id=(sec, sim_peer(k)), device_id_type=MESH,
                ).start()
        if i > 0 and i % 2 == 0:
            t = i // 2 - 1
            if t == 0:
                pl.semaphore_wait(barrier, n_sim - 1 + n_sec - 1)
            if t < staged:
                for k in range(1, 4):
                    to = along_x(k)
                    pltpu.make_async_remote_copy(
                        sendb.at[i - 2, :, block(to), :], first_x.at[k - 1, t], send_sem.at[1], first_sem.at[t, 0],
                        device_id=(sec, z * 4 + to), device_id_type=MESH,
                    ).start()
                    to = along_z(k)
                    pltpu.make_async_remote_copy(
                        sendb.at[i - 1, to], first_z.at[k - 1, t], send_sem.at[7], first_sem.at[t, 1],
                        device_id=(sec, to * 4 + x), device_id_type=MESH,
                    ).start()
            else:
                for k in range(1, n_sim):
                    pltpu.make_async_remote_copy(
                        sendb.at[pl.ds(i - 2, 2), along_z(k // 4), block(along_x(k % 4)), :],
                        straight.at[k - 1, t - staged],
                        send_sem.at[5], straight_sem.at[t - staged],
                        device_id=(sec, sim_peer(k)), device_id_type=MESH,
                    ).start()
    def both_sides(value):
        turned = pltpu.roll(value, width, 1)
        return jnp.where(left16, value, turned), jnp.where(left16, turned, value)

    def about(m_even, m_odd, w_even, w_odd):
        count = jnp.sum(w_even + w_odd, axis=0, keepdims=True)
        mean = jnp.sum(w_even * m_even + w_odd * m_odd, axis=0, keepdims=True) / jnp.maximum(count, 1.0)
        d_even, d_odd = m_even - mean, m_odd - mean
        off = jnp.concatenate([d_even, d_odd], axis=0)
        left = jnp.concatenate([w_even * d_even, w_odd * d_odd], axis=0)
        return count, mean, outer_sum(left, off)[0:width, :]

    def here(c, d):
        return jnp.clip(c - d * cells, 0, cells).astype(F32)

    n_mine = here(n_int, me)
    l_even, l_odd = both_sides(mine / jnp.maximum(n_mine, 1.0))
    dev_count, dev_mean, dev_co = about(l_even, l_odd, here(c_even, me), here(c_odd, me))
    q = qsum + pltpu.roll(qsum, width, 1) + dev_co

    lane32, sub32 = iota((width // 2, 128), 1), iota((width // 2, 128), 0)
    left32 = lane32 < width
    col32 = lane32 % width
    inner32 = col32 < width // 2
    above32 = col32 > sub32

    def folded(m, mean, count):
        top, bottom = m[0:width // 2, :], m[width // 2:width, :]
        kept = jnp.where(inner32 & ~above32, pltpu.roll(bottom, width // 2, 1), top)
        diagonal = jnp.sum(jnp.where(col32 == sub32, top, 0.0), axis=0, keepdims=True)
        info = jnp.where(sub8 == 0, mean, jnp.where(sub8 == 1, count, jnp.where(sub8 == 2, diagonal, 0.0)))
        quarter = width // 4
        return jnp.concatenate(
            [jnp.where(left16, kept[0:quarter, :], kept[quarter:2 * quarter, :]), info], axis=0
        )

    def unfolded(m):
        swapped = pltpu.roll(m[0:pairs, :], width, 1)
        kept = jnp.concatenate(
            [jnp.where(left16, m[0:pairs, :], swapped), jnp.where(left16, swapped, m[0:pairs, :])], axis=0
        )
        turned = jnp.concatenate([kept, kept, kept, kept], axis=0).T[0:width, :]
        first = jnp.where(above32, kept, jnp.where(col32 == sub32, m[pairs + 2:pairs + 3, :], turned[0:width // 2, :]))
        top = jnp.where(inner32, first, kept)
        last = pltpu.roll(jnp.where(above32, turned[0:width // 2, :], kept), width // 2, 1)
        bottom = jnp.where(inner32, turned[width // 2:, :], last)
        return jnp.concatenate([top, bottom], axis=0)

    def third(i):
        return pl.ds(pl.multiple_of(24 * i, 8), 24)

    fold[...] = folded(q, dev_mean, dev_count)
    for k in range(1, n_sec):
        pltpu.make_async_remote_copy(
            fold, qrecv.at[third(sec), :], send_sem.at[2], q_sem,
            device_id=(sec_peer(k), me), device_id_type=MESH,
        ).start()
    qrecv[third(sec), :] = fold[...]

    lane64, sub64 = iota((width, 128), 1), iota((width, 128), 0)
    names = jnp.where(
        ((sub64 % 8) // 2 == (lane64 % width) // n_sim) & (own64[...] == lane64 % n_sim), 1.0, 0.0
    )
    names = jnp.concatenate([names, names], axis=0).T.astype(BF16)

    def merged(ref, n):
        part = ref[0:24, :]
        for s in range(1, n):
            part = part + ref[24 * s:24 * (s + 1), :]
        means = ref[pl.ds(pairs, n, stride=24), :]
        weights = ref[pl.ds(pairs + 1, n, stride=24), :]
        count = jnp.sum(weights, axis=0, keepdims=True)
        mean = jnp.sum(weights * means, axis=0, keepdims=True) / jnp.maximum(count, 1.0)
        gap = means - mean
        return part, mean, count, outer_sum(weights * gap, gap)[0:width, :]

    for t in range(staged):
        few = first_x.at[:, t]
        pltpu.make_async_copy(few, few, first_sem.at[t, 0]).wait()
        few = first_z.at[:, t]
        pltpu.make_async_copy(few, few, first_sem.at[t, 1]).wait()
        part_x[t] = sendb[2 * t, :, block(x), :] + first_x[0, t] + first_x[1, t] + first_x[2, t]
        part_z[t] = sendb[2 * t + 1, z] + first_z[0, t] + first_z[1, t] + first_z[2, t]
    for k in range(1, 4):
        to = along_z(k)
        pltpu.make_async_remote_copy(
            part_x.at[:, to], second_x.at[k - 1], send_sem.at[6], second_sem.at[0],
            device_id=(sec, to * 4 + x), device_id_type=MESH,
        ).start()
        to = along_x(k)
        pltpu.make_async_remote_copy(
            part_z.at[:, block(to), :], second_z.at[k - 1], send_sem.at[8], second_sem.at[1],
            device_id=(sec, z * 4 + to), device_id_type=MESH,
        ).start()

    arrived(qrecv, 24 * (n_sec - 1), q_sem)
    part, part_mean, part_count, part_co = merged(qrecv, n_sec)
    extra = folded(part_co, part_mean, part_count)
    info = jnp.where(sub8 == 2, part[pairs:, :] + extra[pairs:, :], extra[pairs:, :])
    zrecv[third(me), :] = jnp.concatenate([part[0:pairs, :] + extra[0:pairs, :], info], axis=0)
    for k in range(1, n_sim):
        pltpu.make_async_remote_copy(
            zrecv.at[third(me), :], zrecv.at[third(me), :], send_sem.at[3], z_sem,
            device_id=(sec, sim_peer(k)), device_id_type=MESH,
        ).start()

    arrived(sums, n_sim - 1, sums_sem)
    total = sums[0]
    for d in range(1, n_sim):
        total = total + sums[d]
    means = total / n_int.astype(F32)
    turn[pl.ds(0, pairs, stride=2), :] = means
    turn[pl.ds(1, pairs, stride=2), :] = pltpu.roll(means, width, 1)
    mean_out[...] = turn[:, 0:width]

    weighted = []
    for d in range(n_sim):
        n = here(n_int, d)
        gap = sums[d] / jnp.maximum(n, 1.0) - means
        weighted.append(gap * n)
        top = gap.astype(BF16)
        gaps[pairs * d:pairs * (d + 1), :] = top
        gaps[pairs * (n_sim + d):pairs * (n_sim + d + 1), :] = (gap - top.astype(F32)).astype(BF16)
    for r in range(4):
        picked = jnp.dot(gaps[...], sel[:, 128 * r:128 * (r + 1)], preferred_element_type=F32)
        rows = jnp.zeros((pairs, 128), F32)
        for d in range(n_sim):
            one = picked[pairs * d:pairs * (d + 1), :] + picked[pairs * (n_sim + d):pairs * (n_sim + d + 1), :]
            rows = rows + one * weighted[d]
        for pp in range(2):
            corrb[pl.ds(2 * r + pp, half, stride=8), :] = rows[half * pp:half * (pp + 1), :]
    co = corrb[...]
    m_even, m_odd = both_sides(means)
    grp_count, _, grp_co = about(
        m_even, m_odd,
        jnp.where(o_even == me, c_even, 0).astype(F32), jnp.where(o_odd == me, c_odd, 0).astype(F32),
    )
    corrb[...] = grp_co
    between = jnp.where(left32, corrb[pl.ds(0, width // 2, stride=2), :], corrb[pl.ds(1, width // 2, stride=2), :])

    pltpu.make_async_copy(second_x, second_x, second_sem.at[0]).wait()
    pltpu.make_async_copy(second_z, second_z, second_sem.at[1]).wait()
    tiles = []
    for t in range(staged):
        tiles.append(part_x[t, z] + second_x[0, t] + second_x[1, t] + second_x[2, t])
        tiles.append(part_z[t, block(x), :] + second_z[0, t] + second_z[1, t] + second_z[2, t])
    for t in range(half // 2 - staged):
        few = straight.at[:, t]
        pltpu.make_async_copy(few, few, straight_sem.at[t]).wait()
        for u in range(2):
            tile = sendb[2 * (staged + t) + u, z, block(x), :]
            for k in range(n_sim - 1):
                tile = tile + straight[k, t, u]
            tiles.append(tile)
    co = co + jnp.concatenate(tiles, axis=0)
    top = co.astype(BF16)
    low = (co - top.astype(F32)).astype(BF16)
    named = jnp.dot(names, jnp.concatenate([top, low], axis=0), preferred_element_type=F32)
    g = jnp.where(left64, named[0:width, :], named[width:, :])
    g = g + pltpu.roll(g, width, 1)
    gsend[pl.ds(0, n_sim, stride=8), :] = jnp.where(left16, g[0:16, :], g[16:32, :])
    gsend[pl.ds(1, n_sim, stride=8), :] = jnp.where(left16, g[32:48, :], g[48:64, :])
    for k in range(1, n_sim):
        to = sim_peer(k)
        pltpu.make_async_remote_copy(
            gsend.at[block(to), :], grecv.at[block(me), :], send_sem.at[4], g_sem,
            device_id=(sec, to), device_id_type=MESH,
        ).start()
    grecv[block(me), :] = gsend[block(me), :]

    arrived(zrecv, 24 * (n_sim - 1), z_sem)
    part, all_mean, all_count, all_co = merged(zrecv, n_sim)
    gmean_out[...] = all_mean[:, 0:width]
    gcov_out[...] = ((unfolded(part) + all_co) / (all_count - 1.0))[:, 0:width]

    corrb[...] = co / (n64[...] - 1.0)
    for pp in range(2):
        for rr in range(2):
            a = corrb[pl.ds(4 * rr + pp, half, stride=8), :]
            b = corrb[pl.ds(4 * rr + 2 + pp, half, stride=8), :]
            turned = turn if rr == 0 else turn2
            turned[pl.ds(pairs * pp, half, stride=2), :] = jnp.where(left8, a, pltpu.roll(b, width, 1))
            turned[pl.ds(pairs * pp + 1, half, stride=2), :] = jnp.where(left8, pltpu.roll(a, width, 1), b)
    cov_out[:, 0:128] = turn[...]
    cov_out[:, 128:256] = turn2[...]

    arrived(grecv, 8 * (n_sim - 1), g_sem)
    grp[pl.ds(0, n_sim, stride=2), :] = grecv[pl.ds(0, n_sim, stride=8), :]
    grp[pl.ds(1, n_sim, stride=2), :] = grecv[pl.ds(1, n_sim, stride=8), :]
    grp_out[...] = (grp[...] + between) / jnp.maximum(grp_count - 1.0, 1.0)

    arrived(sums, n_sim - 1, send_sem.at[0])
    arrived(first_x, 3, send_sem.at[1])
    arrived(first_z, 3, send_sem.at[7])
    arrived(qrecv, 24 * (n_sec - 1), send_sem.at[2])
    arrived(zrecv, 24 * (n_sim - 1), send_sem.at[3])
    arrived(grecv, 8 * (n_sim - 1), send_sem.at[4])
    arrived(straight, n_sim - 1, send_sem.at[5])
    arrived(second_x, 3, send_sem.at[6])
    arrived(second_z, 3, send_sem.at[8])


def put(n, *refs):
    ins, outs, sem = refs[:n], refs[n:2 * n], refs[2 * n]
    copies = [pltpu.make_async_copy(a, b, sem.at[i]) for i, (a, b) in enumerate(zip(ins, outs))]
    for c in copies:
        c.start()
    for c in copies:
        c.wait()


def solution(mesh):
    n_sec, n_sim = mesh.shape["section"], mesh.shape["sim"]

    def local(state, owner, counts):
        slabs, width, cells = state.shape
        pairs = slabs // 2
        half = pairs // 2
        staged = 2
        vmem = pl.BlockSpec(memory_space=pltpu.VMEM)
        smem = pl.BlockSpec(memory_space=pltpu.SMEM)
        dma = pltpu.SemaphoreType.DMA
        hbm = pl.BlockSpec(memory_space=pltpu.HBM)
        shapes = [
            jax.ShapeDtypeStruct((slabs, width), F32),
            jax.ShapeDtypeStruct((slabs, width * width // n_sim), F32),
            jax.ShapeDtypeStruct((width // 2, 2 * width), F32),
            jax.ShapeDtypeStruct((1, width), F32),
            jax.ShapeDtypeStruct((width, width), F32),
        ]
        found = pl.pallas_call(
            functools.partial(kernel, n_sec, n_sim, width),
            out_shape=shapes,
            in_specs=[hbm] * 3,
            out_specs=[vmem] * 5,
            scratch_shapes=[
                pltpu.VMEM((pairs, 2 * width, cells), F32),
                pltpu.VMEM((2, 2, 4 * width, cells), BF16),
                pltpu.VMEM((128, 128), F32),
                pltpu.VMEM((n_sim, pairs, 128), F32),
                pltpu.VMEM((half, 4, 32, 128), F32),
                pltpu.VMEM((3, staged, 4, 8, 128), F32),
                pltpu.VMEM((3, staged, 32, 128), F32),
                pltpu.VMEM((staged, 4, 8, 128), F32),
                pltpu.VMEM((staged, 32, 128), F32),
                pltpu.VMEM((3, staged, 8, 128), F32),
                pltpu.VMEM((3, staged, 8, 128), F32),
                pltpu.VMEM((n_sim - 1, half // 2 - staged, 2, 8, 128), F32),
                pltpu.VMEM((128, 512), BF16),
                pltpu.VMEM((2 * n_sim * pairs, 128), BF16),
                pltpu.VMEM((24, 128), F32),
                pltpu.VMEM((24 * n_sec, 128), F32),
                pltpu.VMEM((24 * n_sim, 128), F32),
                pltpu.VMEM((8 * n_sim, 128), F32),
                pltpu.VMEM((8 * n_sim, 128), F32),
                pltpu.VMEM((width // 2, 128), F32),
                pltpu.VMEM((width, 128), F32),
                pltpu.VMEM((width, 128), F32),
                pltpu.VMEM((width, 128), jnp.int32),
                pltpu.VMEM((slabs, 128), F32),
                pltpu.VMEM((slabs, 128), F32),
                pltpu.SMEM((slabs,), jnp.int32),
                pltpu.SMEM((slabs,), jnp.int32),
                dma((pairs,)),
                dma((2,)),
                dma((9,)),
                dma(()),
                dma((staged, 2)),
                dma((2,)),
                dma((half // 2 - staged,)),
                dma(()),
                dma(()),
                dma(()),
            ],
            compiler_params=pltpu.CompilerParams(
                collective_id=0, has_side_effects=True, vmem_limit_bytes=32 * 1024 * 1024
            ),
            name="moments",
        )(*(
            pltpu.with_memory_space_constraint(a, pltpu.HBM)
            for a in (state.reshape(pairs, 2 * width, cells), counts, owner.reshape(slabs))
        ))
        mean, cov, grp, gmean, gcov = pl.pallas_call(
            functools.partial(put, 5),
            out_shape=shapes,
            in_specs=[vmem] * 5,
            out_specs=[hbm] * 5,
            scratch_shapes=[dma((5,))],
            compiler_params=pltpu.CompilerParams(vmem_limit_bytes=4 * 1024 * 1024),
            name="put",
        )(*found)
        return mean, cov, grp.reshape(1, width * width), gmean.reshape(width), gcov

    return jax.shard_map(
        local,
        mesh=mesh,
        in_specs=(P("section", None, "sim"), P("section", None), P("section")),
        out_specs=(P("section", None), P("section", "sim"), P(("section", "sim"), None), P(), P()),
        check_vma=False,
    )
```

```python
import functools

import jax
import jax.numpy as jnp
from jax import lax
from jax.experimental import pallas as pl
from jax.experimental.pallas import tpu as pltpu
from jax.sharding import PartitionSpec as P

MESH = pl.DeviceIdType.MESH
F32 = jnp.float32
BF16 = jnp.bfloat16


def dot_rows(a, b):
    return lax.dot_general(a, b, (((1,), (1,)), ((), ())), preferred_element_type=F32)


def outer_sum(a, b):
    a_top, b_top = a.astype(BF16).astype(F32), b.astype(BF16).astype(F32)
    left = jnp.concatenate([a_top, a - a_top, a_top], axis=0)
    right = jnp.concatenate([b_top, b_top, b - b_top], axis=0)
    return jnp.dot(left.T.astype(BF16), right.astype(BF16), preferred_element_type=F32)


def iota(shape, dim):
    return lax.broadcasted_iota(jnp.int32, shape, dim)


def kernel(
    n_sec, n_sim, width,
    state, counts_hbm, owner_hbm,
    mean_out, cov_out, grp_out, gmean_out, gcov_out,
    xv, split, colsum, sums, sendb, first_x, first_z, part_x, part_z, second_x, second_z, straight, sel, gaps, fold, qrecv, zrecv, gsend, grecv, grp, corrb, n64, own64, turn, turn2,
    counts, owner, load_sem, int_sem, send_sem, sums_sem, first_sem, second_sem, straight_sem, q_sem, z_sem, g_sem,
):
    pairs, _, cells = xv.shape
    half = pairs // 2
    sec = lax.axis_index("section")
    me = lax.axis_index("sim")
    z, x = me // 4, me % 4
    base = me * cells

    def sim_peer(k):
        return ((z + k // 4) % 4) * 4 + (x + k % 4) % 4

    def sec_peer(k):
        return (sec + k) % n_sec

    def block(i):
        return pl.ds(pl.multiple_of(8 * i, 8), 8)

    def along_x(k):
        return (x + k) % 4

    def along_z(k):
        return (z + k) % 4

    def arrived(ref, n, sem):
        pltpu.make_async_copy(ref.at[pl.ds(0, n)], ref.at[pl.ds(0, n)], sem).wait()

    def hops(k, n):
        return min(k, n - k)

    far_sim = sorted(range(1, n_sim), key=lambda k: -hops(k // 4, 4) - hops(k % 4, 4))
    far_sec = sorted(range(1, n_sec), key=lambda k: -hops(k, n_sec))

    small = [
        pltpu.make_async_copy(counts_hbm, counts, int_sem.at[0]),
        pltpu.make_async_copy(owner_hbm, owner, int_sem.at[1]),
    ]
    loads = {
        p: pltpu.make_async_copy(state.at[p], xv.at[p], load_sem.at[p])
        for i in range(half) for p in (i, i + half)
    }
    for c in small + list(loads.values()):
        c.start()

    barrier = pltpu.get_barrier_semaphore()
    for k in range(1, n_sim):
        pl.semaphore_signal(barrier, inc=1, device_id=(sec, sim_peer(k)), device_id_type=MESH)
    for k in range(1, n_sec):
        pl.semaphore_signal(barrier, inc=1, device_id=(sec_peer(k), me), device_id_type=MESH)

    for c in small:
        c.wait()

    lane8, sub8 = iota((8, 128), 1), iota((8, 128), 0)
    left8, first8 = lane8 < width, sub8 % 2 == 0
    for i in range(half):
        def spread(ref):
            return jnp.where(
                left8,
                jnp.where(first8, ref[2 * i], ref[2 * (i + half)]),
                jnp.where(first8, ref[2 * i + 1], ref[2 * (i + half) + 1]),
            )
        n64[8 * i:8 * i + 8, :] = spread(counts).astype(F32)
        own64[8 * i:8 * i + 8, :] = spread(owner)
    lane16, sub16 = iota((pairs, 128), 1), iota((pairs, 128), 0)
    left16 = lane16 < width
    c_even = jnp.zeros((pairs, 128), jnp.int32)
    c_odd, o_even, o_odd = c_even, c_even, c_even
    for p in range(pairs):
        here = sub16 == p
        c_even = jnp.where(here, counts[2 * p], c_even)
        c_odd = jnp.where(here, counts[2 * p + 1], c_odd)
        o_even = jnp.where(here, owner[2 * p], o_even)
        o_odd = jnp.where(here, owner[2 * p + 1], o_odd)
    n_int = jnp.where(left16, c_even, c_odd)
    colsum[...] = jnp.zeros((128, 128), F32)
    row128, col128 = iota((128, 128), 0), iota((128, 128), 1)
    for r in range(4):
        sel[:, 128 * r:128 * (r + 1)] = jnp.where(
            row128 == (col128 // width) * width + 4 * me + r, 1.0, 0.0
        ).astype(BF16)

    lane_c = iota((1, cells), 1)
    left64 = iota((width, 128), 1) < width

    def centre(i):
        for pp in range(2):
            p = i + half * pp
            for h in range(2):
                n = jnp.clip(counts[2 * p + h] - base, 0, cells)
                live = lane_c < n
                for r in range(h * width, (h + 1) * width, 16):
                    cell = xv[p, r:r + 16, :]
                    s = jnp.sum(jnp.where(live, cell, 0.0), axis=1, keepdims=True)
                    colsum[r:r + 16, p:p + 1] = s
                    m = s / jnp.maximum(n, 1).astype(F32)
                    c = jnp.where(live, cell - m, 0.0)
                    top = c.astype(BF16)
                    split[i % 2, pp, r:r + 16, :] = top
                    split[i % 2, pp, 2 * width + r:2 * width + r + 16, :] = (c - top.astype(F32)).astype(BF16)

    def multiply(i, qsum):
        for pp in range(2):
            terms = split[i % 2, pp]
            both = dot_rows(terms, terms)
            full = both[0:2 * width, :] + both[2 * width:, :]
            full = full[:, 0:2 * width] + full[:, 2 * width:]
            co = jnp.where(left64, full[0:width, :], full[width:, :])
            qsum = qsum + co
            for j in range(4):
                sendb[i, j, pl.ds(pp, width // 4, stride=2), :] = co[width // 4 * j:width // 4 * (j + 1), :]
        return qsum

    staged = first_x.shape[1]
    qsum = jnp.zeros((width, 128), F32)
    def both_sides(value):
        turned = pltpu.roll(value, width, 1)
        return jnp.where(left16, value, turned), jnp.where(left16, turned, value)

    def about(m_even, m_odd, w_even, w_odd):
        count = jnp.sum(w_even + w_odd, axis=0, keepdims=True)
        mean = jnp.sum(w_even * m_even + w_odd * m_odd, axis=0, keepdims=True) / jnp.maximum(count, 1.0)
        d_even, d_odd = m_even - mean, m_odd - mean
        off = jnp.concatenate([d_even, d_odd], axis=0)
        left = jnp.concatenate([w_even * d_even, w_odd * d_odd], axis=0)
        return count, mean, outer_sum(left, off)[0:width, :]

    def here(c, d):
        return jnp.clip(c - d * cells, 0, cells).astype(F32)

    lane32, sub32 = iota((width // 2, 128), 1), iota((width // 2, 128), 0)
    left32 = lane32 < width
    col32 = lane32 % width
    inner32 = col32 < width // 2
    above32 = col32 > sub32

    def folded(m, mean, count):
        top, bottom = m[0:width // 2, :], m[width // 2:width, :]
        kept = jnp.where(inner32 & ~above32, pltpu.roll(bottom, width // 2, 1), top)
        diagonal = jnp.sum(jnp.where(col32 == sub32, top, 0.0), axis=0, keepdims=True)
        info = jnp.where(sub8 == 0, mean, jnp.where(sub8 == 1, count, jnp.where(sub8 == 2, diagonal, 0.0)))
        quarter = width // 4
        return jnp.concatenate(
            [jnp.where(left16, kept[0:quarter, :], kept[quarter:2 * quarter, :]), info], axis=0
        )

    def unfolded(m):
        swapped = pltpu.roll(m[0:pairs, :], width, 1)
        kept = jnp.concatenate(
            [jnp.where(left16, m[0:pairs, :], swapped), jnp.where(left16, swapped, m[0:pairs, :])], axis=0
        )
        turned = jnp.concatenate([kept, kept, kept, kept], axis=0).T[0:width, :]
        first = jnp.where(above32, kept, jnp.where(col32 == sub32, m[pairs + 2:pairs + 3, :], turned[0:width // 2, :]))
        top = jnp.where(inner32, first, kept)
        last = pltpu.roll(jnp.where(above32, turned[0:width // 2, :], kept), width // 2, 1)
        bottom = jnp.where(inner32, turned[width // 2:, :], last)
        return jnp.concatenate([top, bottom], axis=0)

    def third(i):
        return pl.ds(pl.multiple_of(24 * i, 8), 24)

    for i in range(half + 1):
        if i == 0 or i % 2 == 1:
            for p in range(i, min(half, i + 1 + i % 2)):
                loads[p].wait()
                loads[p + half].wait()
        if i < half:
            centre(i)
        if i > 0 and i != half - 1:
            if i == half:
                qsum = multiply(i - 2, qsum)
            qsum = multiply(i - 1, qsum)
        if i == half:
            mine = colsum[...].T[0:pairs, :]
            sums[me] = mine
            n_mine = here(n_int, me)
            l_even, l_odd = both_sides(mine / jnp.maximum(n_mine, 1.0))
            dev_count, dev_mean, dev_co = about(l_even, l_odd, here(c_even, me), here(c_odd, me))
            q = qsum + pltpu.roll(qsum, width, 1) + dev_co
            fold[...] = folded(q, dev_mean, dev_count)
            for k in far_sec:
                pltpu.make_async_remote_copy(
                    fold, qrecv.at[third(sec), :], send_sem.at[2], q_sem,
                    device_id=(sec_peer(k), me), device_id_type=MESH,
                ).start()
            for k in far_sim:
                pltpu.make_async_remote_copy(
                    sums.at[me], sums.at[me], send_sem.at[0], sums_sem,
                    device_id=(sec, sim_peer(k)), device_id_type=MESH,
                ).start()
        if i > 0 and i % 2 == 0:
            t = i // 2 - 1
            if t == 0:
                pl.semaphore_wait(barrier, n_sim - 1 + n_sec - 1)
            if t < staged:
                for k in range(1, 4):
                    to = along_x(k)
                    pltpu.make_async_remote_copy(
                        sendb.at[i - 2, :, block(to), :], first_x.at[k - 1, t], send_sem.at[1], first_sem.at[t, 0],
                        device_id=(sec, z * 4 + to), device_id_type=MESH,
                    ).start()
                    to = along_z(k)
                    pltpu.make_async_remote_copy(
                        sendb.at[i - 1, to], first_z.at[k - 1, t], send_sem.at[7], first_sem.at[t, 1],
                        device_id=(sec, to * 4 + x), device_id_type=MESH,
                    ).start()
            else:
                for k in far_sim:
                    pltpu.make_async_remote_copy(
                        sendb.at[pl.ds(i - 2, 2), along_z(k // 4), block(along_x(k % 4)), :],
                        straight.at[k - 1, t - staged],
                        send_sem.at[5], straight_sem.at[t - staged],
                        device_id=(sec, sim_peer(k)), device_id_type=MESH,
                    ).start()
    qrecv[third(sec), :] = fold[...]

    lane64, sub64 = iota((width, 128), 1), iota((width, 128), 0)
    names = jnp.where(
        ((sub64 % 8) // 2 == (lane64 % width) // n_sim) & (own64[...] == lane64 % n_sim), 1.0, 0.0
    )
    names = jnp.concatenate([names, names], axis=0).T.astype(BF16)

    def merged(ref, n):
        part = ref[0:24, :]
        for s in range(1, n):
            part = part + ref[24 * s:24 * (s + 1), :]
        means = ref[pl.ds(pairs, n, stride=24), :]
        weights = ref[pl.ds(pairs + 1, n, stride=24), :]
        count = jnp.sum(weights, axis=0, keepdims=True)
        mean = jnp.sum(weights * means, axis=0, keepdims=True) / jnp.maximum(count, 1.0)
        gap = means - mean
        return part, mean, count, outer_sum(weights * gap, gap)[0:width, :]

    for t in range(staged):
        few = first_x.at[:, t]
        pltpu.make_async_copy(few, few, first_sem.at[t, 0]).wait()
        few = first_z.at[:, t]
        pltpu.make_async_copy(few, few, first_sem.at[t, 1]).wait()
        part_x[t] = sendb[2 * t, :, block(x), :] + first_x[0, t] + first_x[1, t] + first_x[2, t]
        part_z[t] = sendb[2 * t + 1, z] + first_z[0, t] + first_z[1, t] + first_z[2, t]
    for k in range(1, 4):
        to = along_z(k)
        pltpu.make_async_remote_copy(
            part_x.at[:, to], second_x.at[k - 1], send_sem.at[6], second_sem.at[0],
            device_id=(sec, to * 4 + x), device_id_type=MESH,
        ).start()
        to = along_x(k)
        pltpu.make_async_remote_copy(
            part_z.at[:, block(to), :], second_z.at[k - 1], send_sem.at[8], second_sem.at[1],
            device_id=(sec, z * 4 + to), device_id_type=MESH,
        ).start()

    arrived(qrecv, 24 * (n_sec - 1), q_sem)
    part, part_mean, part_count, part_co = merged(qrecv, n_sec)
    extra = folded(part_co, part_mean, part_count)
    info = jnp.where(sub8 == 2, part[pairs:, :] + extra[pairs:, :], extra[pairs:, :])
    zrecv[third(me), :] = jnp.concatenate([part[0:pairs, :] + extra[0:pairs, :], info], axis=0)
    for k in far_sim:
        pltpu.make_async_remote_copy(
            zrecv.at[third(me), :], zrecv.at[third(me), :], send_sem.at[3], z_sem,
            device_id=(sec, sim_peer(k)), device_id_type=MESH,
        ).start()

    arrived(sums, n_sim - 1, sums_sem)
    total = sums[0]
    for d in range(1, n_sim):
        total = total + sums[d]
    means = total / n_int.astype(F32)
    turn[pl.ds(0, pairs, stride=2), :] = means
    turn[pl.ds(1, pairs, stride=2), :] = pltpu.roll(means, width, 1)
    mean_out[...] = turn[:, 0:width]

    weighted = []
    for d in range(n_sim):
        n = here(n_int, d)
        gap = sums[d] / jnp.maximum(n, 1.0) - means
        weighted.append(gap * n)
        top = gap.astype(BF16)
        gaps[pairs * d:pairs * (d + 1), :] = top
        gaps[pairs * (n_sim + d):pairs * (n_sim + d + 1), :] = (gap - top.astype(F32)).astype(BF16)
    for r in range(4):
        picked = jnp.dot(gaps[...], sel[:, 128 * r:128 * (r + 1)], preferred_element_type=F32)
        rows = jnp.zeros((pairs, 128), F32)
        for d in range(n_sim):
            one = picked[pairs * d:pairs * (d + 1), :] + picked[pairs * (n_sim + d):pairs * (n_sim + d + 1), :]
            rows = rows + one * weighted[d]
        for pp in range(2):
            corrb[pl.ds(2 * r + pp, half, stride=8), :] = rows[half * pp:half * (pp + 1), :]
    co = corrb[...]
    pltpu.make_async_copy(second_x, second_x, second_sem.at[0]).wait()
    pltpu.make_async_copy(second_z, second_z, second_sem.at[1]).wait()
    tiles = []
    for t in range(staged):
        tiles.append(part_x[t, z] + second_x[0, t] + second_x[1, t] + second_x[2, t])
        tiles.append(part_z[t, block(x), :] + second_z[0, t] + second_z[1, t] + second_z[2, t])
    for t in range(half // 2 - staged):
        few = straight.at[:, t]
        pltpu.make_async_copy(few, few, straight_sem.at[t]).wait()
        for u in range(2):
            tile = sendb[2 * (staged + t) + u, z, block(x), :]
            for k in range(n_sim - 1):
                tile = tile + straight[k, t, u]
            tiles.append(tile)
    co = co + jnp.concatenate(tiles, axis=0)
    top = co.astype(BF16)
    low = (co - top.astype(F32)).astype(BF16)
    named = jnp.dot(names, jnp.concatenate([top, low], axis=0), preferred_element_type=F32)
    g = jnp.where(left64, named[0:width, :], named[width:, :])
    g = g + pltpu.roll(g, width, 1)
    gsend[:, 0, :] = jnp.where(left16, g[0:16, :], g[16:32, :])
    gsend[:, 1, :] = jnp.where(left16, g[32:48, :], g[48:64, :])
    for k in far_sim:
        to = sim_peer(k)
        pltpu.make_async_remote_copy(
            gsend.at[to], grecv.at[me], send_sem.at[4], g_sem,
            device_id=(sec, to), device_id_type=MESH,
        ).start()
    grecv[me] = gsend[me]

    m_even, m_odd = both_sides(means)
    grp_count, _, grp_co = about(
        m_even, m_odd,
        jnp.where(o_even == me, c_even, 0).astype(F32), jnp.where(o_odd == me, c_odd, 0).astype(F32),
    )
    corrb[...] = grp_co
    between = jnp.where(left32, corrb[pl.ds(0, width // 2, stride=2), :], corrb[pl.ds(1, width // 2, stride=2), :])

    arrived(zrecv, 24 * (n_sim - 1), z_sem)
    part, all_mean, all_count, all_co = merged(zrecv, n_sim)
    gmean_out[...] = all_mean[:, 0:width]
    gcov_out[...] = ((unfolded(part) + all_co) / (all_count - 1.0))[:, 0:width]

    corrb[...] = co / (n64[...] - 1.0)
    for pp in range(2):
        for rr in range(2):
            a = corrb[pl.ds(4 * rr + pp, half, stride=8), :]
            b = corrb[pl.ds(4 * rr + 2 + pp, half, stride=8), :]
            turned = turn if rr == 0 else turn2
            turned[pl.ds(pairs * pp, half, stride=2), :] = jnp.where(left8, a, pltpu.roll(b, width, 1))
            turned[pl.ds(pairs * pp + 1, half, stride=2), :] = jnp.where(left8, pltpu.roll(a, width, 1), b)
    cov_out[:, 0:128] = turn[...]
    cov_out[:, 128:256] = turn2[...]

    arrived(grecv, n_sim - 1, g_sem)
    grp[pl.ds(0, n_sim, stride=2), :] = grecv[:, 0, :]
    grp[pl.ds(1, n_sim, stride=2), :] = grecv[:, 1, :]
    grp_out[...] = (grp[...] + between) / jnp.maximum(grp_count - 1.0, 1.0)

    arrived(sums, n_sim - 1, send_sem.at[0])
    arrived(first_x, 3, send_sem.at[1])
    arrived(first_z, 3, send_sem.at[7])
    arrived(qrecv, 24 * (n_sec - 1), send_sem.at[2])
    arrived(zrecv, 24 * (n_sim - 1), send_sem.at[3])
    arrived(grecv, n_sim - 1, send_sem.at[4])
    arrived(straight, n_sim - 1, send_sem.at[5])
    arrived(second_x, 3, send_sem.at[6])
    arrived(second_z, 3, send_sem.at[8])


def put(n, *refs):
    ins, outs, sem = refs[:n], refs[n:2 * n], refs[2 * n]
    copies = [pltpu.make_async_copy(a, b, sem.at[i]) for i, (a, b) in enumerate(zip(ins, outs))]
    for c in copies:
        c.start()
    for c in copies:
        c.wait()


def solution(mesh):
    n_sec, n_sim = mesh.shape["section"], mesh.shape["sim"]

    def local(state, owner, counts):
        slabs, width, cells = state.shape
        pairs = slabs // 2
        half = pairs // 2
        staged = 2
        vmem = pl.BlockSpec(memory_space=pltpu.VMEM)
        smem = pl.BlockSpec(memory_space=pltpu.SMEM)
        dma = pltpu.SemaphoreType.DMA
        hbm = pl.BlockSpec(memory_space=pltpu.HBM)
        shapes = [
            jax.ShapeDtypeStruct((slabs, width), F32),
            jax.ShapeDtypeStruct((slabs, width * width // n_sim), F32),
            jax.ShapeDtypeStruct((width // 2, 2 * width), F32),
            jax.ShapeDtypeStruct((1, width), F32),
            jax.ShapeDtypeStruct((width, width), F32),
        ]
        found = pl.pallas_call(
            functools.partial(kernel, n_sec, n_sim, width),
            out_shape=shapes,
            in_specs=[hbm] * 3,
            out_specs=[vmem] * 5,
            scratch_shapes=[
                pltpu.VMEM((pairs, 2 * width, cells), F32),
                pltpu.VMEM((2, 2, 4 * width, cells), BF16),
                pltpu.VMEM((128, 128), F32),
                pltpu.VMEM((n_sim, pairs, 128), F32),
                pltpu.VMEM((half, 4, 32, 128), F32),
                pltpu.VMEM((3, staged, 4, 8, 128), F32),
                pltpu.VMEM((3, staged, 32, 128), F32),
                pltpu.VMEM((staged, 4, 8, 128), F32),
                pltpu.VMEM((staged, 32, 128), F32),
                pltpu.VMEM((3, staged, 8, 128), F32),
                pltpu.VMEM((3, staged, 8, 128), F32),
                pltpu.VMEM((n_sim - 1, half // 2 - staged, 2, 8, 128), F32),
                pltpu.VMEM((128, 512), BF16),
                pltpu.VMEM((2 * n_sim * pairs, 128), BF16),
                pltpu.VMEM((24, 128), F32),
                pltpu.VMEM((24 * n_sec, 128), F32),
                pltpu.VMEM((24 * n_sim, 128), F32),
                pltpu.VMEM((n_sim, 2, 128), F32),
                pltpu.VMEM((n_sim, 2, 128), F32),
                pltpu.VMEM((width // 2, 128), F32),
                pltpu.VMEM((width, 128), F32),
                pltpu.VMEM((width, 128), F32),
                pltpu.VMEM((width, 128), jnp.int32),
                pltpu.VMEM((slabs, 128), F32),
                pltpu.VMEM((slabs, 128), F32),
                pltpu.SMEM((slabs,), jnp.int32),
                pltpu.SMEM((slabs,), jnp.int32),
                dma((pairs,)),
                dma((2,)),
                dma((9,)),
                dma(()),
                dma((staged, 2)),
                dma((2,)),
                dma((half // 2 - staged,)),
                dma(()),
                dma(()),
                dma(()),
            ],
            compiler_params=pltpu.CompilerParams(
                collective_id=0, has_side_effects=True, vmem_limit_bytes=32 * 1024 * 1024
            ),
            name="moments",
        )(*(
            pltpu.with_memory_space_constraint(a, pltpu.HBM)
            for a in (state.reshape(pairs, 2 * width, cells), counts, owner.reshape(slabs))
        ))
        mean, cov, grp, gmean, gcov = pl.pallas_call(
            functools.partial(put, 5),
            out_shape=shapes,
            in_specs=[vmem] * 5,
            out_specs=[hbm] * 5,
            scratch_shapes=[dma((5,))],
            compiler_params=pltpu.CompilerParams(vmem_limit_bytes=4 * 1024 * 1024),
            name="put",
        )(*found)
        return mean, cov, grp.reshape(1, width * width), gmean.reshape(width), gcov

    return jax.shard_map(
        local,
        mesh=mesh,
        in_specs=(P("section", None, "sim"), P("section", None), P("section")),
        out_specs=(P("section", None), P("section", "sim"), P(("section", "sim"), None), P(), P()),
        check_vma=False,
    )
```

```python
import functools

import jax
import jax.numpy as jnp
from jax import lax
from jax.experimental import pallas as pl
from jax.experimental.pallas import tpu as pltpu
from jax.sharding import PartitionSpec as P

MESH = pl.DeviceIdType.MESH
F32 = jnp.float32
BF16 = jnp.bfloat16


def dot_rows(a, b):
    return lax.dot_general(a, b, (((1,), (1,)), ((), ())), preferred_element_type=F32)


def outer_sum(a, b):
    a_top, b_top = a.astype(BF16).astype(F32), b.astype(BF16).astype(F32)
    left = jnp.concatenate([a_top, a - a_top, a_top], axis=0)
    right = jnp.concatenate([b_top, b_top, b - b_top], axis=0)
    return jnp.dot(left.T.astype(BF16), right.astype(BF16), preferred_element_type=F32)


def iota(shape, dim):
    return lax.broadcasted_iota(jnp.int32, shape, dim)


def kernel(
    n_sec, n_sim, width,
    state, counts_hbm, owner_hbm,
    mean_out, cov_out, grp_out, gmean_out, gcov_out,
    xv, split, colsum, sums, sendb, first_x, first_z, part_x, part_z, second_x, second_z, straight, sel, gaps, fold, qrecv, zrecv, gsend, grecv, grp, corrb, n64, own64, turn, turn2,
    counts, owner, load_sem, int_sem, send_sem, sums_sem, first_sem, second_sem, straight_sem, q_sem, z_sem, g_sem,
):
    pairs, _, cells = xv.shape
    half = pairs // 2
    sec = lax.axis_index("section")
    me = lax.axis_index("sim")
    z, x = me // 4, me % 4
    base = me * cells

    def sim_peer(k):
        return ((z + k // 4) % 4) * 4 + (x + k % 4) % 4

    def sec_peer(k):
        return (sec + k) % n_sec

    def block(i):
        return pl.ds(pl.multiple_of(8 * i, 8), 8)

    def along_x(k):
        return (x + k) % 4

    def along_z(k):
        return (z + k) % 4

    def arrived(ref, n, sem):
        pltpu.make_async_copy(ref.at[pl.ds(0, n)], ref.at[pl.ds(0, n)], sem).wait()

    def hops(k, n):
        return min(k, n - k)

    far_sim = sorted(range(1, n_sim), key=lambda k: -hops(k // 4, 4) - hops(k % 4, 4))
    far_sec = sorted(range(1, n_sec), key=lambda k: -hops(k, n_sec))

    small = [
        pltpu.make_async_copy(counts_hbm, counts, int_sem.at[0]),
        pltpu.make_async_copy(owner_hbm, owner, int_sem.at[1]),
    ]
    loads = {
        p: pltpu.make_async_copy(state.at[p], xv.at[p], load_sem.at[p])
        for i in range(half) for p in (i, i + half)
    }
    for c in small + list(loads.values()):
        c.start()

    barrier = pltpu.get_barrier_semaphore()
    for k in range(1, n_sim):
        pl.semaphore_signal(barrier, inc=1, device_id=(sec, sim_peer(k)), device_id_type=MESH)
    for k in range(1, n_sec):
        pl.semaphore_signal(barrier, inc=1, device_id=(sec_peer(k), me), device_id_type=MESH)

    for c in small:
        c.wait()

    lane8, sub8 = iota((8, 128), 1), iota((8, 128), 0)
    left8, first8 = lane8 < width, sub8 % 2 == 0
    for i in range(half):
        def spread(ref):
            return jnp.where(
                left8,
                jnp.where(first8, ref[2 * i], ref[2 * (i + half)]),
                jnp.where(first8, ref[2 * i + 1], ref[2 * (i + half) + 1]),
            )
        n64[8 * i:8 * i + 8, :] = spread(counts).astype(F32)
        own64[8 * i:8 * i + 8, :] = spread(owner)
    lane16, sub16 = iota((pairs, 128), 1), iota((pairs, 128), 0)
    left16 = lane16 < width
    c_even = jnp.zeros((pairs, 128), jnp.int32)
    c_odd, o_even, o_odd = c_even, c_even, c_even
    for p in range(pairs):
        here = sub16 == p
        c_even = jnp.where(here, counts[2 * p], c_even)
        c_odd = jnp.where(here, counts[2 * p + 1], c_odd)
        o_even = jnp.where(here, owner[2 * p], o_even)
        o_odd = jnp.where(here, owner[2 * p + 1], o_odd)
    n_int = jnp.where(left16, c_even, c_odd)
    colsum[...] = jnp.zeros((128, 128), F32)
    row128, col128 = iota((128, 128), 0), iota((128, 128), 1)
    for r in range(4):
        sel[:, 128 * r:128 * (r + 1)] = jnp.where(
            row128 == (col128 // width) * width + 4 * me + r, 1.0, 0.0
        ).astype(BF16)

    lane_c = iota((1, cells), 1)
    left64 = iota((width, 128), 1) < width

    def centre(i):
        for pp in range(2):
            p = i + half * pp
            for h in range(2):
                n = jnp.clip(counts[2 * p + h] - base, 0, cells)
                live = lane_c < n
                weight = jnp.where(live, 1.0, 0.0)
                for r in range(h * width, (h + 1) * width, 16):
                    cell = xv[p, r:r + 16, :]
                    s = jnp.sum(cell * weight, axis=1, keepdims=True)
                    colsum[r:r + 16, p:p + 1] = s
                    m = s / jnp.maximum(n, 1).astype(F32)
                    c = jnp.where(live, cell - m, 0.0)
                    top = c.astype(BF16)
                    split[i % 2, pp, r:r + 16, :] = top
                    split[i % 2, pp, 2 * width + r:2 * width + r + 16, :] = (c - top.astype(F32)).astype(BF16)

    def multiply(i, qsum):
        for pp in range(2):
            terms = split[i % 2, pp]
            both = dot_rows(terms, terms)
            full = both[0:2 * width, :] + both[2 * width:, :]
            full = full[:, 0:2 * width] + full[:, 2 * width:]
            co = jnp.where(left64, full[0:width, :], full[width:, :])
            qsum = qsum + co
            for j in range(4):
                sendb[i, j, pl.ds(pp, width // 4, stride=2), :] = co[width // 4 * j:width // 4 * (j + 1), :]
        return qsum

    staged = first_x.shape[1]
    qsum = jnp.zeros((width, 128), F32)
    def both_sides(value):
        turned = pltpu.roll(value, width, 1)
        return jnp.where(left16, value, turned), jnp.where(left16, turned, value)

    def about(m_even, m_odd, w_even, w_odd):
        count = jnp.sum(w_even + w_odd, axis=0, keepdims=True)
        mean = jnp.sum(w_even * m_even + w_odd * m_odd, axis=0, keepdims=True) / jnp.maximum(count, 1.0)
        d_even, d_odd = m_even - mean, m_odd - mean
        off = jnp.concatenate([d_even, d_odd], axis=0)
        left = jnp.concatenate([w_even * d_even, w_odd * d_odd], axis=0)
        return count, mean, outer_sum(left, off)[0:width, :]

    def here(c, d):
        return jnp.clip(c - d * cells, 0, cells).astype(F32)

    lane32, sub32 = iota((width // 2, 128), 1), iota((width // 2, 128), 0)
    left32 = lane32 < width
    col32 = lane32 % width
    inner32 = col32 < width // 2
    above32 = col32 > sub32

    def folded(m, mean, count):
        top, bottom = m[0:width // 2, :], m[width // 2:width, :]
        kept = jnp.where(inner32 & ~above32, pltpu.roll(bottom, width // 2, 1), top)
        diagonal = jnp.sum(jnp.where(col32 == sub32, top, 0.0), axis=0, keepdims=True)
        info = jnp.where(sub8 == 0, mean, jnp.where(sub8 == 1, count, jnp.where(sub8 == 2, diagonal, 0.0)))
        quarter = width // 4
        return jnp.concatenate(
            [jnp.where(left16, kept[0:quarter, :], kept[quarter:2 * quarter, :]), info], axis=0
        )

    def unfolded(m):
        swapped = pltpu.roll(m[0:pairs, :], width, 1)
        kept = jnp.concatenate(
            [jnp.where(left16, m[0:pairs, :], swapped), jnp.where(left16, swapped, m[0:pairs, :])], axis=0
        )
        turned = jnp.concatenate([kept, kept, kept, kept], axis=0).T[0:width, :]
        first = jnp.where(above32, kept, jnp.where(col32 == sub32, m[pairs + 2:pairs + 3, :], turned[0:width // 2, :]))
        top = jnp.where(inner32, first, kept)
        last = pltpu.roll(jnp.where(above32, turned[0:width // 2, :], kept), width // 2, 1)
        bottom = jnp.where(inner32, turned[width // 2:, :], last)
        return jnp.concatenate([top, bottom], axis=0)

    def third(i):
        return pl.ds(pl.multiple_of(24 * i, 8), 24)

    for i in range(half + 1):
        if i == 0 or i % 2 == 1:
            for p in range(i, min(half, i + 1 + i % 2)):
                loads[p].wait()
                loads[p + half].wait()
        if i < half:
            centre(i)
        if i > 0 and i != half - 1:
            if i == half:
                qsum = multiply(i - 2, qsum)
            qsum = multiply(i - 1, qsum)
        if i == half:
            mine = colsum[...].T[0:pairs, :]
            sums[me] = mine
            n_mine = here(n_int, me)
            l_even, l_odd = both_sides(mine / jnp.maximum(n_mine, 1.0))
            dev_count, dev_mean, dev_co = about(l_even, l_odd, here(c_even, me), here(c_odd, me))
            for k in far_sim:
                pltpu.make_async_remote_copy(
                    sums.at[me], sums.at[me], send_sem.at[0], sums_sem,
                    device_id=(sec, sim_peer(k)), device_id_type=MESH,
                ).start()
            q = qsum + pltpu.roll(qsum, width, 1) + dev_co
            fold[...] = folded(q, dev_mean, dev_count)
            for k in far_sec:
                pltpu.make_async_remote_copy(
                    fold, qrecv.at[third(sec), :], send_sem.at[2], q_sem,
                    device_id=(sec_peer(k), me), device_id_type=MESH,
                ).start()
        if i > 0 and i % 2 == 0:
            t = i // 2 - 1
            if t == 0:
                pl.semaphore_wait(barrier, n_sim - 1 + n_sec - 1)
            if t < staged:
                for k in (2, 1, 3):
                    to = along_x(k)
                    pltpu.make_async_remote_copy(
                        sendb.at[i - 2, :, block(to), :], first_x.at[k - 1, t], send_sem.at[1], first_sem.at[t, 0],
                        device_id=(sec, z * 4 + to), device_id_type=MESH,
                    ).start()
                    to = along_z(k)
                    pltpu.make_async_remote_copy(
                        sendb.at[i - 1, to], first_z.at[k - 1, t], send_sem.at[7], first_sem.at[t, 1],
                        device_id=(sec, to * 4 + x), device_id_type=MESH,
                    ).start()
            else:
                for k in far_sim:
                    pltpu.make_async_remote_copy(
                        sendb.at[pl.ds(i - 2, 2), along_z(k // 4), block(along_x(k % 4)), :],
                        straight.at[k - 1, t - staged],
                        send_sem.at[5], straight_sem.at[t - staged],
                        device_id=(sec, sim_peer(k)), device_id_type=MESH,
                    ).start()
    qrecv[third(sec), :] = fold[...]

    lane64, sub64 = iota((width, 128), 1), iota((width, 128), 0)
    names = jnp.where(
        ((sub64 % 8) // 2 == (lane64 % width) // n_sim) & (own64[...] == lane64 % n_sim), 1.0, 0.0
    )
    names = jnp.concatenate([names, names], axis=0).T.astype(BF16)

    def merged(ref, n):
        part = ref[0:24, :]
        for s in range(1, n):
            part = part + ref[24 * s:24 * (s + 1), :]
        means = ref[pl.ds(pairs, n, stride=24), :]
        weights = ref[pl.ds(pairs + 1, n, stride=24), :]
        count = jnp.sum(weights, axis=0, keepdims=True)
        mean = jnp.sum(weights * means, axis=0, keepdims=True) / jnp.maximum(count, 1.0)
        gap = means - mean
        return part, mean, count, outer_sum(weights * gap, gap)[0:width, :]

    for t in range(staged):
        few = first_x.at[:, t]
        pltpu.make_async_copy(few, few, first_sem.at[t, 0]).wait()
        few = first_z.at[:, t]
        pltpu.make_async_copy(few, few, first_sem.at[t, 1]).wait()
        part_x[t] = sendb[2 * t, :, block(x), :] + first_x[0, t] + first_x[1, t] + first_x[2, t]
        part_z[t] = sendb[2 * t + 1, z] + first_z[0, t] + first_z[1, t] + first_z[2, t]
    for k in (2, 1, 3):
        to = along_z(k)
        pltpu.make_async_remote_copy(
            part_x.at[:, to], second_x.at[k - 1], send_sem.at[6], second_sem.at[0],
            device_id=(sec, to * 4 + x), device_id_type=MESH,
        ).start()
        to = along_x(k)
        pltpu.make_async_remote_copy(
            part_z.at[:, block(to), :], second_z.at[k - 1], send_sem.at[8], second_sem.at[1],
            device_id=(sec, z * 4 + to), device_id_type=MESH,
        ).start()

    arrived(qrecv, 24 * (n_sec - 1), q_sem)
    part, part_mean, part_count, part_co = merged(qrecv, n_sec)
    extra = folded(part_co, part_mean, part_count)
    info = jnp.where(sub8 == 2, part[pairs:, :] + extra[pairs:, :], extra[pairs:, :])
    zrecv[third(me), :] = jnp.concatenate([part[0:pairs, :] + extra[0:pairs, :], info], axis=0)
    for k in far_sim:
        pltpu.make_async_remote_copy(
            zrecv.at[third(me), :], zrecv.at[third(me), :], send_sem.at[3], z_sem,
            device_id=(sec, sim_peer(k)), device_id_type=MESH,
        ).start()

    arrived(sums, n_sim - 1, sums_sem)
    total = sums[0]
    for d in range(1, n_sim):
        total = total + sums[d]
    means = total / n_int.astype(F32)
    turn[pl.ds(0, pairs, stride=2), :] = means
    turn[pl.ds(1, pairs, stride=2), :] = pltpu.roll(means, width, 1)
    mean_out[...] = turn[:, 0:width]

    weighted = []
    for d in range(n_sim):
        n = here(n_int, d)
        gap = sums[d] / jnp.maximum(n, 1.0) - means
        weighted.append(gap * n)
        top = gap.astype(BF16)
        gaps[pairs * d:pairs * (d + 1), :] = top
        gaps[pairs * (n_sim + d):pairs * (n_sim + d + 1), :] = (gap - top.astype(F32)).astype(BF16)
    for r in range(4):
        picked = jnp.dot(gaps[...], sel[:, 128 * r:128 * (r + 1)], preferred_element_type=F32)
        rows = jnp.zeros((pairs, 128), F32)
        for d in range(n_sim):
            one = picked[pairs * d:pairs * (d + 1), :] + picked[pairs * (n_sim + d):pairs * (n_sim + d + 1), :]
            rows = rows + one * weighted[d]
        for pp in range(2):
            corrb[pl.ds(2 * r + pp, half, stride=8), :] = rows[half * pp:half * (pp + 1), :]
    co = corrb[...]
    pltpu.make_async_copy(second_x, second_x, second_sem.at[0]).wait()
    pltpu.make_async_copy(second_z, second_z, second_sem.at[1]).wait()
    tiles = []
    for t in range(staged):
        tiles.append(part_x[t, z] + second_x[0, t] + second_x[1, t] + second_x[2, t])
        tiles.append(part_z[t, block(x), :] + second_z[0, t] + second_z[1, t] + second_z[2, t])
    for t in range(half // 2 - staged):
        few = straight.at[:, t]
        pltpu.make_async_copy(few, few, straight_sem.at[t]).wait()
        for u in range(2):
            tile = sendb[2 * (staged + t) + u, z, block(x), :]
            for k in range(n_sim - 1):
                tile = tile + straight[k, t, u]
            tiles.append(tile)
    co = co + jnp.concatenate(tiles, axis=0)
    top = co.astype(BF16)
    low = (co - top.astype(F32)).astype(BF16)
    named = jnp.dot(names, jnp.concatenate([top, low], axis=0), preferred_element_type=F32)
    g = jnp.where(left64, named[0:width, :], named[width:, :])
    g = g + pltpu.roll(g, width, 1)
    gsend[:, 0, :] = jnp.where(left16, g[0:16, :], g[16:32, :])
    gsend[:, 1, :] = jnp.where(left16, g[32:48, :], g[48:64, :])
    for k in far_sim:
        to = sim_peer(k)
        pltpu.make_async_remote_copy(
            gsend.at[to], grecv.at[me], send_sem.at[4], g_sem,
            device_id=(sec, to), device_id_type=MESH,
        ).start()
    grecv[me] = gsend[me]

    m_even, m_odd = both_sides(means)
    grp_count, _, grp_co = about(
        m_even, m_odd,
        jnp.where(o_even == me, c_even, 0).astype(F32), jnp.where(o_odd == me, c_odd, 0).astype(F32),
    )
    corrb[...] = grp_co
    between = jnp.where(left32, corrb[pl.ds(0, width // 2, stride=2), :], corrb[pl.ds(1, width // 2, stride=2), :])

    arrived(zrecv, 24 * (n_sim - 1), z_sem)
    part, all_mean, all_count, all_co = merged(zrecv, n_sim)
    gmean_out[...] = all_mean[:, 0:width]
    gcov_out[...] = ((unfolded(part) + all_co) / (all_count - 1.0))[:, 0:width]

    corrb[...] = co / (n64[...] - 1.0)
    for pp in range(2):
        for rr in range(2):
            a = corrb[pl.ds(4 * rr + pp, half, stride=8), :]
            b = corrb[pl.ds(4 * rr + 2 + pp, half, stride=8), :]
            turned = turn if rr == 0 else turn2
            turned[pl.ds(pairs * pp, half, stride=2), :] = jnp.where(left8, a, pltpu.roll(b, width, 1))
            turned[pl.ds(pairs * pp + 1, half, stride=2), :] = jnp.where(left8, pltpu.roll(a, width, 1), b)
    cov_out[:, 0:128] = turn[...]
    cov_out[:, 128:256] = turn2[...]

    arrived(grecv, n_sim - 1, g_sem)
    grp[pl.ds(0, n_sim, stride=2), :] = grecv[:, 0, :]
    grp[pl.ds(1, n_sim, stride=2), :] = grecv[:, 1, :]
    grp_out[...] = (grp[...] + between) / jnp.maximum(grp_count - 1.0, 1.0)

    arrived(sums, n_sim - 1, send_sem.at[0])
    arrived(first_x, 3, send_sem.at[1])
    arrived(first_z, 3, send_sem.at[7])
    arrived(qrecv, 24 * (n_sec - 1), send_sem.at[2])
    arrived(zrecv, 24 * (n_sim - 1), send_sem.at[3])
    arrived(grecv, n_sim - 1, send_sem.at[4])
    arrived(straight, n_sim - 1, send_sem.at[5])
    arrived(second_x, 3, send_sem.at[6])
    arrived(second_z, 3, send_sem.at[8])


def put(n, *refs):
    ins, outs, sem = refs[:n], refs[n:2 * n], refs[2 * n]
    copies = [pltpu.make_async_copy(a, b, sem.at[i]) for i, (a, b) in enumerate(zip(ins, outs))]
    for c in copies:
        c.start()
    for c in copies:
        c.wait()


def solution(mesh):
    n_sec, n_sim = mesh.shape["section"], mesh.shape["sim"]

    def local(state, owner, counts):
        slabs, width, cells = state.shape
        pairs = slabs // 2
        half = pairs // 2
        staged = 2
        vmem = pl.BlockSpec(memory_space=pltpu.VMEM)
        smem = pl.BlockSpec(memory_space=pltpu.SMEM)
        dma = pltpu.SemaphoreType.DMA
        hbm = pl.BlockSpec(memory_space=pltpu.HBM)
        shapes = [
            jax.ShapeDtypeStruct((slabs, width), F32),
            jax.ShapeDtypeStruct((slabs, width * width // n_sim), F32),
            jax.ShapeDtypeStruct((width // 2, 2 * width), F32),
            jax.ShapeDtypeStruct((1, width), F32),
            jax.ShapeDtypeStruct((width, width), F32),
        ]
        found = pl.pallas_call(
            functools.partial(kernel, n_sec, n_sim, width),
            out_shape=shapes,
            in_specs=[hbm] * 3,
            out_specs=[vmem] * 5,
            scratch_shapes=[
                pltpu.VMEM((pairs, 2 * width, cells), F32),
                pltpu.VMEM((2, 2, 4 * width, cells), BF16),
                pltpu.VMEM((128, 128), F32),
                pltpu.VMEM((n_sim, pairs, 128), F32),
                pltpu.VMEM((half, 4, 32, 128), F32),
                pltpu.VMEM((3, staged, 4, 8, 128), F32),
                pltpu.VMEM((3, staged, 32, 128), F32),
                pltpu.VMEM((staged, 4, 8, 128), F32),
                pltpu.VMEM((staged, 32, 128), F32),
                pltpu.VMEM((3, staged, 8, 128), F32),
                pltpu.VMEM((3, staged, 8, 128), F32),
                pltpu.VMEM((n_sim - 1, half // 2 - staged, 2, 8, 128), F32),
                pltpu.VMEM((128, 512), BF16),
                pltpu.VMEM((2 * n_sim * pairs, 128), BF16),
                pltpu.VMEM((24, 128), F32),
                pltpu.VMEM((24 * n_sec, 128), F32),
                pltpu.VMEM((24 * n_sim, 128), F32),
                pltpu.VMEM((n_sim, 2, 128), F32),
                pltpu.VMEM((n_sim, 2, 128), F32),
                pltpu.VMEM((width // 2, 128), F32),
                pltpu.VMEM((width, 128), F32),
                pltpu.VMEM((width, 128), F32),
                pltpu.VMEM((width, 128), jnp.int32),
                pltpu.VMEM((slabs, 128), F32),
                pltpu.VMEM((slabs, 128), F32),
                pltpu.SMEM((slabs,), jnp.int32),
                pltpu.SMEM((slabs,), jnp.int32),
                dma((pairs,)),
                dma((2,)),
                dma((9,)),
                dma(()),
                dma((staged, 2)),
                dma((2,)),
                dma((half // 2 - staged,)),
                dma(()),
                dma(()),
                dma(()),
            ],
            compiler_params=pltpu.CompilerParams(
                collective_id=0, has_side_effects=True, vmem_limit_bytes=32 * 1024 * 1024
            ),
            name="moments",
        )(*(
            pltpu.with_memory_space_constraint(a, pltpu.HBM)
            for a in (state.reshape(pairs, 2 * width, cells), counts, owner.reshape(slabs))
        ))
        mean, cov, grp, gmean, gcov = pl.pallas_call(
            functools.partial(put, 5),
            out_shape=shapes,
            in_specs=[vmem] * 5,
            out_specs=[hbm] * 5,
            scratch_shapes=[dma((5,))],
            compiler_params=pltpu.CompilerParams(vmem_limit_bytes=4 * 1024 * 1024),
            name="put",
        )(*found)
        return mean, cov, grp.reshape(1, width * width), gmean.reshape(width), gcov

    return jax.shard_map(
        local,
        mesh=mesh,
        in_specs=(P("section", None, "sim"), P("section", None), P("section")),
        out_specs=(P("section", None), P("section", "sim"), P(("section", "sim"), None), P(), P()),
        check_vma=False,
    )
```
